16 devices in a mesh: data: 2 (over y, z), cp: 8 (over x, core).
Axes of the slice: x: 4, y: 2, z: 1, core: 2. Of those that a mesh axis runs over, the one named last changes fastest.
The devices are a block of a 4x4x8 slice.
Arguments:
- x_tokens: bfloat16 [32, 2048, 4096], P('data', 'cp'), parts along dimension 0
- positions: int32 [32, 2048], P('data', 'cp'), parts along dimension 0
- w_query: bfloat16 [4096, 4096], replicated
- w_key: bfloat16 [4096, 1024], replicated
- w_value: bfloat16 [4096, 1024], replicated
- w_out: bfloat16 [4096, 4096], replicated
Outputs:
- output: bfloat16 [32, 2048, 4096], P('data', 'cp'), parts along dimension 0
There are 2 independent parts. The reference program is written for one: setup_inputs(seed, part) draws one part's arguments, and reference() takes and returns one part's arrays. A program takes and returns all parts, laid end to end along the dimension named above; an argument that names none is the same for every part.
All inputs are finite; a program needn't handle non-finite values.
Results may differ from the reference program's by a relative error of at most 0.0046917.
Values are sent between devices in bfloat16 or wider.
A program may use at most 768 MiB of HBM per device.

```python
import jax
import jax.numpy as jnp
from jax import lax

BATCH_PART = 16
SEQ_LEN = 2048
CP_SIZE = 8
MODEL_DIM = 4096
Q_HEADS = 32
KV_HEADS = 8
HEAD_DIM = 128
ROPE_BASE = 500000
WALK_SEG = 16

GROUP_SIZE = Q_HEADS // KV_HEADS
HALF_LEN = SEQ_LEN // (2 * CP_SIZE)
BLOCK_LEN = min(HALF_LEN, 256)
BLOCK_COUNT = SEQ_LEN // BLOCK_LEN


def to_stored_order(seq_arr):
    tail_dims = seq_arr.shape[2:]
    blocks = seq_arr.reshape((BATCH_PART, 2 * CP_SIZE, HALF_LEN) + tail_dims)
    front_part = blocks[:, :CP_SIZE]
    back_part = jnp.flip(blocks[:, CP_SIZE:], axis=1)
    return jnp.stack([front_part, back_part], axis=2).reshape(seq_arr.shape)


def setup_inputs(seed: int = 0, part: int = 0) -> dict:
    root_key = jax.random.key(seed)
    k_query, k_key, k_value, k_out, k_part = jax.random.split(root_key, 5)
    part_key = jax.random.fold_in(k_part, part)
    k_noise, k_mean, k_walk, k_gap, k_start = jax.random.split(part_key, 5)
    seg_count = SEQ_LEN // WALK_SEG
    walk_steps = jax.random.normal(k_walk, (BATCH_PART, seg_count, MODEL_DIM), jnp.float32)
    walk_path = jnp.repeat(jnp.cumsum(walk_steps, axis=1) * (seg_count ** -0.5), WALK_SEG, axis=1)
    row_mean = jax.random.normal(k_mean, (BATCH_PART, 1, MODEL_DIM), jnp.float32)
    token_noise = jax.random.normal(k_noise, (BATCH_PART, SEQ_LEN, MODEL_DIM), jnp.float32)
    x_seq = 0.5 * token_noise + 0.5 * row_mean + walk_path
    pos_gaps = jax.random.randint(k_gap, (BATCH_PART, SEQ_LEN), 1, 4, dtype=jnp.int32)
    start_pos = jax.random.randint(k_start, (BATCH_PART, 1), 0, 1024, dtype=jnp.int32)
    pos_seq = start_pos + jnp.cumsum(pos_gaps, axis=1, dtype=jnp.int32)
    q_cols = Q_HEADS * HEAD_DIM
    kv_cols = KV_HEADS * HEAD_DIM
    w_query = (jax.random.normal(k_query, (MODEL_DIM, q_cols), jnp.float32) * MODEL_DIM ** -0.5).astype(jnp.bfloat16)
    w_key = (jax.random.normal(k_key, (MODEL_DIM, kv_cols), jnp.float32) * MODEL_DIM ** -0.5).astype(jnp.bfloat16)
    w_value = (jax.random.normal(k_value, (MODEL_DIM, kv_cols), jnp.float32) * MODEL_DIM ** -0.5).astype(jnp.bfloat16)
    w_out = (jax.random.normal(k_out, (q_cols, MODEL_DIM), jnp.float32) * (2.0 * q_cols ** -0.5)).astype(jnp.bfloat16)
    return {'x_tokens': to_stored_order(x_seq).astype(jnp.bfloat16), 'positions': to_stored_order(pos_seq), 'w_query': w_query, 'w_key': w_key, 'w_value': w_value, 'w_out': w_out}


def apply_rope(head_vecs, positions):
    half_dim = HEAD_DIM // 2
    inv_freq = 1.0 / (ROPE_BASE ** (jnp.arange(0, HEAD_DIM, 2, dtype=jnp.float32) / HEAD_DIM))
    angles = positions.astype(jnp.float32)[:, :, None] * inv_freq
    tab_shape = angles.shape[:2] + (1,) * (head_vecs.ndim - 3) + (half_dim,)
    cosine = jnp.cos(angles).reshape(tab_shape)
    sine_tab = jnp.sin(angles).reshape(tab_shape)
    lower_half = head_vecs[..., :half_dim].astype(jnp.float32)
    upper_half = head_vecs[..., half_dim:].astype(jnp.float32)
    rotated = jnp.concatenate([lower_half * cosine - upper_half * sine_tab, upper_half * cosine + lower_half * sine_tab], axis=-1)
    return rotated.astype(jnp.bfloat16)


def reference(x_tokens, positions, w_query, w_key, w_value, w_out):
    score_scale = HEAD_DIM ** -0.5
    mask_fill = -1e30
    flat_x = x_tokens.reshape(BATCH_PART * SEQ_LEN, MODEL_DIM)
    q_proj = jnp.dot(flat_x, w_query, preferred_element_type=jnp.float32).astype(jnp.bfloat16)
    k_proj = jnp.dot(flat_x, w_key, preferred_element_type=jnp.float32).astype(jnp.bfloat16)
    v_proj = jnp.dot(flat_x, w_value, preferred_element_type=jnp.float32).astype(jnp.bfloat16)
    q_rot = apply_rope(q_proj.reshape(BATCH_PART, SEQ_LEN, KV_HEADS, GROUP_SIZE, HEAD_DIM), positions)
    k_rot = apply_rope(k_proj.reshape(BATCH_PART, SEQ_LEN, KV_HEADS, HEAD_DIM), positions)
    v_rows = v_proj.reshape(BATCH_PART, SEQ_LEN, KV_HEADS, HEAD_DIM)
    q_blocks = jnp.moveaxis(q_rot.reshape(BATCH_PART, BLOCK_COUNT, BLOCK_LEN, KV_HEADS, GROUP_SIZE, HEAD_DIM), 1, 0)
    k_blocks = jnp.moveaxis(k_rot.reshape(BATCH_PART, BLOCK_COUNT, BLOCK_LEN, KV_HEADS, HEAD_DIM), 1, 0)
    v_blocks = jnp.moveaxis(v_rows.reshape(BATCH_PART, BLOCK_COUNT, BLOCK_LEN, KV_HEADS, HEAD_DIM), 1, 0)
    pos_blocks = jnp.moveaxis(positions.reshape(BATCH_PART, BLOCK_COUNT, BLOCK_LEN), 1, 0)

    def query_block(block_in):
        q_blk, q_pos = block_in
        q_wide = q_blk.astype(jnp.float32)

        def key_step(carry_state, key_in):
            m_run, l_run, acc_run = carry_state
            k_blk, v_blk, k_pos = key_in
            scores = jnp.einsum('bqhgd,bkhd->bhgqk', q_wide, k_blk.astype(jnp.float32)) * score_scale
            allowed = (k_pos[:, None, :] <= q_pos[:, :, None])[:, None, None]
            scores = jnp.where(allowed, scores, mask_fill)
            m_new = jnp.maximum(m_run, jnp.max(scores, axis=-1))
            exp_w = jnp.where(allowed, jnp.exp(scores - m_new[..., None]), 0.0)
            rescale = jnp.exp(m_run - m_new)
            l_new = rescale * l_run + jnp.sum(exp_w, axis=-1)
            pv_part = jnp.einsum('bhgqk,bkhd->bhgqd', exp_w.astype(jnp.bfloat16).astype(jnp.float32), v_blk.astype(jnp.float32))
            return (m_new, l_new, rescale[..., None] * acc_run + pv_part), None

        state_shape = (BATCH_PART, KV_HEADS, GROUP_SIZE, BLOCK_LEN)
        init_state = (jnp.full(state_shape, mask_fill, jnp.float32), jnp.zeros(state_shape, jnp.float32), jnp.zeros(state_shape + (HEAD_DIM,), jnp.float32))
        final_state, _ = lax.scan(key_step, init_state, (k_blocks, v_blocks, pos_blocks))
        attn_out = (final_state[2] / final_state[1][..., None]).astype(jnp.bfloat16)
        return attn_out.transpose(0, 3, 1, 2, 4)

    attn_all = lax.map(query_block, (q_blocks, pos_blocks))
    attn_rows = jnp.moveaxis(attn_all, 0, 1).reshape(BATCH_PART * SEQ_LEN, Q_HEADS * HEAD_DIM)
    out_proj = jnp.dot(attn_rows, w_out, preferred_element_type=jnp.float32).reshape(BATCH_PART, SEQ_LEN, MODEL_DIM)
    return (x_tokens.astype(jnp.float32) + out_proj).astype(jnp.bfloat16)
```

```python
import functools
import math

import jax
import jax.numpy as jnp
from jax import lax
from jax.experimental import pallas as pl
from jax.experimental.pallas import tpu as pltpu
from jax.sharding import PartitionSpec as P

HEAD_DIM = 128
ROPE_BASE = 500000
MASK_FILL = -1e30
EXP_SCALE = float(HEAD_DIM ** -0.5 * math.log2(math.e))
CORES = 2
ROWS = 2
TILE = 1024
GROUP = 4
PAIR = 256
VMEM_LIMIT = 66_000_000
LAG = 3
DELAY = 3
BACK = (6, 9)
EPI = 3
AHEAD = 6
SINGLE = 3
SPREAD = 3
COST = (4.7, 4.65, 1.6, 22.8, 1.75, 18.0)
SPLIT = 4
R1, L1, X0, R2, L2, X1, X2, X3 = range(8)
f32, bf16 = jnp.float32, jnp.bfloat16
div, rem = lax.div, lax.rem


def rope_tables(positions):
    half = HEAD_DIM // 2
    inv_freq = 1.0 / (ROPE_BASE ** (jnp.arange(0, HEAD_DIM, 2, dtype=f32) / HEAD_DIM))
    half_len = positions.shape[1] // 2
    pos = positions.astype(f32)
    front = jnp.broadcast_to(pos[:, :half_len, None], pos[:, :half_len].shape + (half,))
    back = jnp.broadcast_to(pos[:, half_len:, None], front.shape)
    angles = (jnp.concatenate([front, back], axis=-1) * jnp.concatenate([inv_freq, inv_freq])).reshape(-1, HEAD_DIM)
    return jnp.cos(angles), jnp.sin(angles)


def attn_scratch(cp, half_len):
    steps, fixed = cp + 1, cp // 2
    keys = 2 * half_len
    groups = lambda *shape: [pltpu.VMEM(shape, f32), pltpu.VMEM(shape, f32)]
    return [
        pltpu.VMEM((2, cp, 2, 2, GROUP, HEAD_DIM, half_len), bf16),
        *groups(steps, keys, PAIR),
        *groups(1 + len(BACK), HEAD_DIM, PAIR),
        *groups(fixed, HEAD_DIM, PAIR),
        *groups(2, 1, PAIR),
        *groups(2, 1, PAIR),
        pltpu.VMEM((2, keys, half_len), f32),
    ]


def attn_init(cp, scratch):
    _, _, _, _, _, pv0, pv1, _, _, _, _, bias = scratch
    keys, half_len = bias.shape[1:]
    kpos = lax.broadcasted_iota(jnp.int32, (keys, half_len), 0)
    qpos = lax.broadcasted_iota(jnp.int32, (keys, half_len), 1)
    for ref in (pv0, pv1):
        ref[ref.shape[0] - 1] = jnp.zeros(ref.shape[1:], f32)
    for p in range(2):
        bias[p] = jnp.where(kpos - qpos <= p * half_len, 0.0, MASK_FILL)


def attn_step(n, cp, my, q_ref, put, scratch):
    kvbuf, sc0, sc1, ac0, ac1, pv0, pv1, mx0, mx1, sm0, sm1, bias = scratch
    sbuf, acc, pvb, mst, lst = (sc0, sc1), (ac0, ac1), (pv0, pv1), (mx0, mx1), (sm0, sm1)
    steps, fixed = cp + 1, cp // 2
    half_len = kvbuf.shape[6]
    here = (rem(div(n, GROUP), 2), rem(n, GROUP))
    before = jnp.maximum(n - 1, 0)
    behind_ = (rem(div(before, GROUP), 2), rem(before, GROUP))
    nf, par = div(my, 2) + 1, rem(my, 2)

    def plan(t):
        if t == 0:
            return 0, nf - 1
        if t >= fixed:
            return 1, t - nf
        front = t < nf
        return jnp.where(front, 0, 1), jnp.where(front, t - 1, t - nf)

    def places(u):
        out = []
        for j in (2 * u, 2 * u + 1):
            front = j < cp
            out.append((jnp.where(front, j, 2 * cp - 1 - j), jnp.where(front, 0, 1)))
        return out

    plans = [plan(t) for t in range(steps)]
    locs = [places(u) for _, u in plans]
    low = jnp.full((1, PAIR), MASK_FILL, f32)
    zero = jnp.zeros((1, PAIR), f32)

    def scores(t, g):
        slot, e = here
        k = jnp.concatenate([kvbuf[slot, s, 0, f, e] for s, f in locs[t]], axis=0)
        s = lax.dot_general(k, q_ref[plans[t][0], 2 * g:2 * g + 2].reshape(PAIR, HEAD_DIM), (((1,), (1,)), ((), ())), preferred_element_type=f32)
        if t == 0 or t == steps - 1:
            b = bias[par if t == 0 else 1 - par]
            s = s + jnp.concatenate([b, b], axis=1)
        sbuf[g][t] = s
        return jnp.max(s, axis=0, keepdims=True)

    def finish_max(g, ms):
        front_max, back_max = ms[0], functools.reduce(jnp.maximum, ms[fixed:])
        for t in range(1, fixed):
            front = t < nf
            front_max = jnp.maximum(front_max, jnp.where(front, ms[t], low))
            back_max = jnp.maximum(back_max, jnp.where(front, low, ms[t]))
        mst[g][0] = front_max
        mst[g][1] = back_max

    def soft(t, g, behind):
        m = mst[g][plans[t][0]]
        if behind is not None:
            m = jnp.maximum(m, jnp.minimum(behind, MASK_FILL))
        p = jnp.exp2((sbuf[g][t] - m) * EXP_SCALE)
        return jnp.sum(p, axis=0, keepdims=True), p.astype(bf16)

    def weighted(ts, ps, at):
        slot, e = at
        vals = jnp.concatenate([kvbuf[slot, s, 1, f, e] for t in ts for s, f in locs[t]], axis=1)
        p = ps[0] if len(ps) == 1 else jnp.concatenate(ps, axis=0)
        return lax.dot_general(vals, p, (((1,), (0,)), ((), ())), preferred_element_type=f32)

    def epilogue(g):
        for half in range(2):
            inv = 1.0 / lst[g][half]
            for e in range(PAIR // HEAD_DIM):
                lanes = slice(e * half_len, (e + 1) * half_len)
                o = acc[g][half, :, lanes]
                for i in range(1, len(BACK) if half else 1):
                    o = o + acc[g][1 + i, :, lanes]
                for t in range(1, fixed):
                    mine = t < nf if half == 0 else t >= nf
                    o = o + pvb[g][jnp.where(mine, t - 1, fixed - 1), :, lanes]
                put(half, g * (PAIR // HEAD_DIM) + e, (o * inv[:, lanes]).astype(bf16).T)
                yield

    def put_weighted(g, ts, ps, at):
        out = weighted(ts, ps, at)
        if ts[0] == 0:
            acc[g][0] = out
        elif ts[0] < fixed:
            pvb[g][ts[0] - 1] = out
        else:
            acc[g][1 + BACK.index(ts[-1] + 1)] = out

    pending = []

    def drain(limit):
        while len(pending) > limit:
            put_weighted(*pending.pop(0))

    for g1, g2, at in ((0, 1, behind_), (1, 0, here)):
        epi = epilogue(g1)
        ms, lf, lb, held = [], None, zero, []
        for t in range(steps):
            ms.append(scores(t, g1))
            l, p = soft(t, g2, ms[t - LAG] if t >= LAG else None)
            if t < fixed:
                front = t < nf
                lf = l if t == 0 else lf + jnp.where(front, l, zero)
                lb = lb if t == 0 else lb + jnp.where(front, zero, l)
                pending.append((g2, [t], [p], at))
            else:
                lb = lb + l
                held.append(p)
                if t + 1 in BACK:
                    pending.append((g2, list(range(t + 1 - len(held), t + 1)), held, at))
                    held = []
            drain(DELAY)
            if t >= EPI:
                next(epi, None)
        lst[g2][0] = lf
        lst[g2][1] = lb
        finish_max(g1, ms)
        for _ in epi:
            pass
    drain(0)


def plan_steps(chunks, n_proj, n_out, per_chunk, send_at):
    seq = [('P', i) for i in range(AHEAD * n_proj)]
    p, o = AHEAD * n_proj, 0
    for c in range(chunks):
        seq += [('A', c * per_chunk + i) for i in range(per_chunk)]
        if c >= chunks - SINGLE:
            seq.append(('S', (c + 1) * per_chunk))
        end = n_out * (c + 1 if c >= chunks - SINGLE else c)
        seq += [('O', i) for i in range(o, end)]
        o = end
        if p < chunks * n_proj:
            seq += [('P', p + i) for i in range(SPREAD)]
            p += SPREAD
            if p == chunks * n_proj:
                seq.append(('F', 0))
    units = [(c * ROWS, ROWS) for c in range(chunks - SINGLE)] + [(i, 1) for i in range((chunks - SINGLE) * ROWS, chunks * ROWS)]
    first_use = [seq.index(('A', row * per_chunk // ROWS)) for row, _ in units]
    proj, out, att, wire, inner, now = COST
    took = {'P': proj, 'O': out, 'A': att, 'S': att, 'F': 0.6}
    hops = {'own': [], 'one': [], 'two': [], 'three': [], 'in': []}
    link, core, got1, got2, sent = 0.0, 0.0, {}, {}, -1
    for step, (kind, i) in enumerate(seq):
        if step and seq[step - 1][0] == 'P' and seq[step - 1][1] % n_proj == send_at:
            sent = seq[step - 1][1] // n_proj
            hops['own'].append(step)
        must = max((u for u in range(len(units)) if first_use[u] <= step + 1), default=-1)
        done = lambda name: len(hops[name])
        while done('one') < len(units) or done('two') < len(units):
            u = done('two')
            if done('one') < min(u + 2, len(units)):
                u = done('one')
                if units[u][0] // ROWS > sent:
                    break
                link = max(now, link) + wire * units[u][1]
                got1[u] = link
                hops['one'].append(step)
            else:
                if now < got1[u] + 3 and u > must:
                    break
                now = max(now, got1[u])
                link = max(now, link) + wire * units[u][1] / 2
                core = max(now, core) + 2 * inner * units[u][1]
                got2[u] = max(link, core)
                hops['two'].append(step)
        while done('three') < done('two') and (got2[done('three')] + 3 <= now or done('three') <= must):
            u = done('three')
            now = max(now, got2[u])
            core = max(now, core) + inner * units[u][1]
            hops['three'].append(step)
        now += took[kind]
    for u in range(len(units)):
        hops['in'].append(first_use[u] - 1)
    return seq, units, hops


def layer(mesh, x_loc, cosine, sine, w_query, w_key, w_value, w_out):
    cp = mesh.shape['cp']
    rows, tok_rows, depth = x_loc.shape
    half_len = tok_rows // 2
    inner, kv_cols = w_query.shape[1], w_key.shape[1]
    heads = kv_cols // HEAD_DIM
    group_cols = inner // heads
    per_tile, fold = TILE // HEAD_DIM, TILE // HEAD_DIM // GROUP
    toks = ROWS * tok_rows
    chunks = rows // ROWS
    kt, qt, n_out = kv_cols // TILE, inner // TILE, depth // TILE
    n_proj = 2 * kt + qt
    per_chunk = ROWS * heads
    total = rows * heads
    n_groups = heads // GROUP
    assert n_groups == 2
    assert depth == w_query.shape[0] and group_cols == 2 * PAIR and n_proj % SPREAD == 0 and rows % ROWS == 0
    assert kt == 1 and SPREAD > 2 * kt and group_cols == GROUP * HEAD_DIM and cp // CORES == 4
    seq, units, hops = plan_steps(chunks, n_proj, n_out, per_chunk, 2 * kt)
    n_steps = len(seq)
    loops = (chunks - AHEAD) * n_proj // SPREAD
    assert 2 <= loops <= chunks - SINGLE
    first_a = seq.index(('A', 0))
    second_a = seq.index(('A', per_chunk))
    flush = seq.index(('F', 0))
    period = per_chunk + n_out + SPREAD
    ends = [i for i in range(flush, n_steps) if i == flush or seq[i][0] != seq[i - 1][0]] + [n_steps]
    tail = [(start, seq[start]) for start in ends[:-1]]
    base = n_proj * AHEAD + SPREAD
    both = n_out + SPREAD
    last_both = base + both * (loops - 1)
    n_tiles = (n_proj + n_out) * chunks

    def pick(cases, other):
        for cond, val in reversed(cases):
            other = jnp.where(cond, val, other)
        return other

    def kern(x_hbm, cos_ref, sin_ref, wq_hbm, wk_hbm, wv_hbm, wo_hbm, y_hbm, kv_hbm, q_hbm,
             wbuf, xbuf, xres, raw, stage, oscr, ybuf, qbuf,
             wsem, xsem, rsem, osem, ysem, qsem, kvsem, send_sem, recv_sem, *attn):
        s = pl.program_id(0)
        my = lax.axis_index('cp')
        chip, core = div(my, CORES), rem(my, CORES)
        chips = cp // CORES

        def device(chip_shift, core_shift=0):
            return rem(chip + chip_shift, chips) * CORES + rem(core + core_shift, CORES)

        nxt, far, prv, mate = device(1), device(2), device(chips - 1), device(0, 1)

        a, r = 1 + div(s - second_a, period), rem(s - second_a, period)
        r0 = s - first_a
        kinds = {'A': 0, 'S': 1, 'O': 2, 'P': 3, 'F': 4}
        parts = [
            (s < first_a, 3, s),
            (s < first_a + per_chunk, 0, r0),
            (s < second_a, 3, s - per_chunk),
            (s < flush, jnp.where(r < per_chunk, 0, jnp.where(r < per_chunk + n_out, 2, 3)),
             jnp.where(r < per_chunk, a * per_chunk + r,
                       jnp.where(r < per_chunk + n_out, (a - 1) * n_out + r - per_chunk, AHEAD * n_proj + a * SPREAD + r - per_chunk - n_out))),
        ]
        for (start, (what, i)), (stop, _) in zip(tail, tail[1:] + [(n_steps, None)]):
            parts.append((s < stop, kinds[what], s + (i - start)))
        kind = pick([(c, k) for c, k, _ in parts[:-1]], parts[-1][1])
        num = pick([(c, i) for c, _, i in parts[:-1]], parts[-1][2])
        is_new, is_skew, is_out, is_proj, is_flush = (kind == k for k in range(5))
        is_head = kind < 2
        n = oidx = pidx = num
        oc, col = div(oidx, n_out), rem(oidx, n_out)
        pc, pt = div(pidx, n_proj), rem(pidx, n_proj)
        tile_p = jnp.where(pidx < base, pidx, base + div(pidx - base, SPREAD) * both + n_out + rem(pidx - base, SPREAD))
        tile_o = jnp.where(oc < loops - 1, base + oc * both + col, last_both + oidx - (loops - 1) * n_out)

        def row_ds(c):
            return pl.ds(c * ROWS, ROWS)

        def load_tile(j):
            slot = rem(j, 2)
            u = j - base
            v = j - last_both
            only_out = j >= last_both
            is_p = jnp.logical_or(j < base, jnp.logical_and(jnp.logical_not(only_out), rem(u, both) >= n_out))
            p = rem(jnp.where(j < base, j, base + div(u, both) * SPREAD + rem(u, both) - n_out), n_proj)
            o_col = jnp.where(only_out, rem(v, n_out), rem(u, both))
            o_chunk = jnp.where(only_out, loops - 1 + div(v, n_out), div(u, both))

            def start(w_hbm, tile_col):
                cols = pl.ds(pl.multiple_of(tile_col * TILE, TILE), TILE)
                part = w_hbm.shape[0] // SPLIT
                for i in range(SPLIT):
                    ks = pl.ds(i * part, part)
                    pltpu.make_async_copy(w_hbm.at[ks, cols], wbuf.at[slot, ks], wsem.at[slot]).start()

            @pl.when(jnp.logical_and(is_p, p < kt))
            def _():
                start(wk_hbm, p)

            @pl.when(jnp.logical_and(is_p, jnp.logical_and(p >= kt, p < 2 * kt)))
            def _():
                start(wv_hbm, p - kt)

            @pl.when(jnp.logical_and(is_p, p >= 2 * kt))
            def _():
                start(wq_hbm, p - 2 * kt)

            @pl.when(jnp.logical_not(is_p))
            def _():
                start(wo_hbm, o_col)
                load_res(o_chunk, o_col, slot).start()

        def load_res(c, tile_col, slot):
            cols = pl.ds(pl.multiple_of(tile_col * TILE, TILE), TILE)
            return pltpu.make_async_copy(x_hbm.at[row_ds(c), :, cols], xres.at[slot], rsem.at[slot])

        def next_tile(j):
            @pl.when(j + 1 < n_tiles)
            def _():
                load_tile(j + 1)
            slot = rem(j, 2)
            pltpu.make_async_copy(wo_hbm.at[:, pl.ds(0, TILE)], wbuf.at[slot], wsem.at[slot]).wait()
            return slot

        def load_x(c):
            return pltpu.make_async_copy(x_hbm.at[row_ds(c)], xbuf.at[rem(c, 2)], xsem.at[rem(c, 2)])

        def load_q(m):
            return pltpu.make_async_copy(q_hbm.at[div(m, heads), rem(m, heads)], qbuf.at[rem(m, 2)], qsem.at[rem(m, 2)])

        def load_kv(g):
            slot = rem(g, 2)
            return [pltpu.make_async_copy(kv_hbm.at[div(g, n_groups), src, rem(g, n_groups)], attn[0].at[slot, src], kvsem.at[slot]) for src in range(cp)]

        def wait_kv(g):
            slot = rem(g, 2)
            pltpu.make_async_copy(kv_hbm.at[0, :, 0], attn[0].at[slot], kvsem.at[slot]).wait()

        def store_y(c, tile_col, slot):
            cols = pl.ds(pl.multiple_of(tile_col * TILE, TILE), TILE)
            return pltpu.make_async_copy(ybuf.at[slot], y_hbm.at[row_ds(c), :, cols], ysem.at[slot])

        def hop(kind, row, size, part=None):
            rs = pl.ds(row, size)
            src, to = {R1: (my, nxt), L1: (my, prv), X0: (my, mate), R2: (prv, nxt), L2: (nxt, prv), X1: (nxt, mate), X2: (far, mate), X3: (prv, mate)}[kind]
            ref = kv_hbm.at[rs, src]
            if kind in (R2, L2):
                group = 0 if kind == R2 else 1
                ref = kv_hbm.at[rs, src, group] if part is None else kv_hbm.at[rs, src, group, part]
            elif part is not None:
                ref = kv_hbm.at[rs, src, part]
            sem = 2 * row + (part or 0)
            return pltpu.make_async_remote_copy(src_ref=ref, dst_ref=ref, send_sem=send_sem.at[kind, sem], recv_sem=recv_sem.at[kind, sem],
                                                device_id={'cp': to}, device_id_type=pl.DeviceIdType.MESH)

        def ring(kinds, row, size, act):
            @pl.when(core == 0)
            def _():
                near(kinds, row, size, act)

            @pl.when(jnp.logical_and(core != 0, size == 1))
            def _():
                for kind in kinds:
                    for part in range(2):
                        act(hop(kind, row, 1, part))

            @pl.when(jnp.logical_and(core != 0, size != 1))
            def _():
                for kind in kinds:
                    for i in range(ROWS):
                        act(hop(kind, row + i, 1))

        def near(kinds, row, size, act):
            @pl.when(size == 1)
            def _():
                for kind in kinds:
                    act(hop(kind, row, 1))

            @pl.when(size != 1)
            def _():
                for kind in kinds:
                    act(hop(kind, row, ROWS))

        start, received, left = (lambda c: c.start()), (lambda c: c.wait_recv()), (lambda c: c.wait_send())

        def hop_one(row, size):
            ring((R1, L1), row, size, start)
            near((X0,), row, size, start)

        def hop_two(row, size):
            ring((R1, L1), row, size, received)
            ring((R2, L2), row, size, start)
            near((X1, X3), row, size, start)

        def hop_three(row, size):
            ring((R2, L2), row, size, received)
            near((X2,), row, size, start)

        def arrive(row, size):
            near((X0, X1, X3, X2), row, size, received)
            ring((R1, L1, R2, L2), row, size, left)
            near((X0, X1, X3, X2), row, size, left)
            for copy in load_kv(row * n_groups):
                copy.start()

            @pl.when(row == 0)
            def _():
                load_q(0).start()

        def own_stored(row, size):
            first = div(row, ROWS) * n_proj
            wait_store(first)
            wait_store(first + 1)

        def unit_hops(lo, hi):
            for name, act in (('own', own_stored), ('two', hop_two), ('one', hop_one), ('three', hop_three), ('in', arrive)):
                due = [(step, (u * ROWS, ROWS) if name == 'own' else units[u]) for u, step in enumerate(hops[name]) if lo <= step < hi]
                if not due:
                    continue
                row, size = pick([(s == step, row) for step, (row, _) in due], -1), pick([(s == step, size) for step, (_, size) in due], ROWS)

                @pl.when(row >= 0)
                def _(row=row, size=size, act=act):
                    act(row, size)

        @pl.when(s == 0)
        def _():
            barrier = pltpu.get_barrier_semaphore()
            for to in (nxt, prv, mate):
                pl.semaphore_signal(barrier, inc=1, device_id={'cp': to}, device_id_type=pl.DeviceIdType.MESH)
            load_x(0).start()
            load_tile(0)
            attn_init(cp, attn)
            pl.semaphore_wait(barrier, 3)

        def store_tile(p):
            c, tile, slot = div(p, n_proj), rem(p, n_proj), rem(p, 2)
            rs = row_ds(c)

            @pl.when(tile < 2)
            def _():
                pltpu.make_async_copy(stage.at[slot], kv_hbm.at[rs, my, :, tile], osem.at[slot]).start()

            @pl.when(tile >= 2)
            def _():
                pltpu.make_async_copy(stage.at[slot], q_hbm.at[rs, pl.ds((tile - 2) * fold, fold)], osem.at[slot]).start()

        def wait_store(p):
            slot = rem(p, 2)
            pltpu.make_async_copy(stage.at[slot], q_hbm.at[pl.ds(0, ROWS), pl.ds(0, fold)], osem.at[slot]).wait()

        def rope_epilogue(p):
            c, slot = div(p, n_proj), rem(p, 2)
            is_v = rem(p, n_proj) == 1
            low_lanes = lax.broadcasted_iota(jnp.int32, (half_len, HEAD_DIM), 1) < HEAD_DIM // 2
            for i in range(ROWS):
                ts = pl.ds(pl.multiple_of((c * ROWS + i) * half_len, half_len), half_len)
                cos, sin = cos_ref[ts], sin_ref[ts]
                cos_r, sin_r = pltpu.roll(cos, HEAD_DIM // 2, 1), pltpu.roll(sin, HEAD_DIM // 2, 1)
                for half in range(2):
                    cos_h = jnp.where(low_lanes, cos, cos_r) if half == 0 else jnp.where(low_lanes, cos_r, cos)
                    sin_h = jnp.where(low_lanes, -sin, sin_r) if half == 0 else jnp.where(low_lanes, -sin_r, sin)
                    rs = slice(i * tok_rows + half * half_len, i * tok_rows + (half + 1) * half_len)
                    for e in range(per_tile):
                        vals = raw[rs, e * HEAD_DIM:(e + 1) * HEAD_DIM]
                        wide = vals.astype(f32)
                        turned = (wide * cos_h + pltpu.roll(wide, HEAD_DIM // 2, 1) * sin_h).astype(bf16)
                        stage[slot, i, e // GROUP, half, e % GROUP] = jnp.where(is_v, vals.T, turned)

        @pl.when(is_proj)
        def _():
            next_tile(tile_p)

            @pl.when(jnp.logical_and(pidx >= 3, jnp.logical_or(pt < 3, pt > 4)))
            def _():
                wait_store(pidx - 3)

            @pl.when(pt == 0)
            def _():
                load_x(pc).wait()

            @pl.when(jnp.logical_and(pt == 1, pc + 1 < chunks))
            def _():
                load_x(pc + 1).start()

        spans = 4
        for i in range(spans):
            lo, hi = n_steps * i // spans, n_steps * (i + 1) // spans

            @pl.when(jnp.logical_and(s >= lo, s < hi))
            def _(lo=lo, hi=hi):
                unit_hops(lo, hi)

        @pl.when(is_proj)
        def _():
            rope_epilogue(jnp.maximum(pidx - 1, 0))
            x = xbuf[rem(pc, 2)].reshape(toks, depth)
            raw[...] = jnp.dot(x, wbuf[rem(tile_p, 2)], preferred_element_type=f32).astype(bf16)

            @pl.when(pidx >= 1)
            def _():
                store_tile(pidx - 1)

        @pl.when(is_flush)
        def _():
            end = n_proj * chunks
            wait_store(end - 3)
            rope_epilogue(end - 1)
            store_tile(end - 1)
            wait_store(end - 2)
            wait_store(end - 1)

        @pl.when(is_head)
        def _():
            g = div(n, GROUP)

            @pl.when(jnp.logical_and(n < total, jnp.logical_or(is_skew, jnp.logical_or(rem(n, per_chunk) != 0, n <= total - SINGLE * per_chunk))))
            def _():
                load_q(n).wait()

            @pl.when(is_new)
            def _():
                @pl.when(n + 1 < total)
                def _():
                    load_q(n + 1).start()

                @pl.when(rem(n, GROUP) == 0)
                def _():
                    wait_kv(g)

                fresh = jnp.logical_or(rem(g + 1, ROWS * n_groups) == 0, jnp.logical_and(g + 1 >= (rows - SINGLE * ROWS) * n_groups, rem(g + 1, n_groups) == 0))

                @pl.when(jnp.logical_and(rem(n, GROUP) == 1, jnp.logical_not(fresh)))
                def _():
                    for copy in load_kv(g + 1):
                        copy.start()

            m = jnp.maximum(n - 1, 0)
            o_slot = rem(div(m, per_chunk), 2)
            row, head = rem(div(m, heads), ROWS), rem(m, heads)

            def put(half, j, val):
                rs = pl.ds(pl.multiple_of(row * tok_rows + half * half_len, half_len), half_len)
                cs = pl.ds(pl.multiple_of(head * group_cols + j * HEAD_DIM, HEAD_DIM), HEAD_DIM)
                oscr[o_slot, rs, cs] = val

            attn_step(n, cp, my, qbuf.at[rem(n, 2)], put, attn)

        @pl.when(is_out)
        def _():
            slot = next_tile(tile_o)
            y_slot = rem(oidx, 2)
            load_res(oc, col, slot).wait()

            @pl.when(oidx >= 2)
            def _():
                store_y(0, 0, y_slot).wait()

            out = jnp.dot(oscr[rem(oc, 2)], wbuf[slot], preferred_element_type=f32)
            ybuf[y_slot] = (xres[slot].astype(f32) + out.reshape(ROWS, tok_rows, TILE)).astype(bf16)
            store_y(oc, col, y_slot).start()

            @pl.when(oidx == n_out * chunks - 1)
            def _():
                store_y(0, 0, 1 - y_slot).wait()
                store_y(0, 0, y_slot).wait()

    any_spec = pl.BlockSpec(memory_space=pl.ANY)
    flops = 2 * rows * tok_rows * depth * (2 * inner + 2 * kv_cols) + 8 * total * (cp + 1) * half_len * group_cols * HEAD_DIM * 2
    y, _, _ = pl.pallas_call(
        kern,
        name='layer',
        grid=(n_steps,),
        in_specs=[any_spec, pl.BlockSpec(memory_space=pltpu.VMEM), pl.BlockSpec(memory_space=pltpu.VMEM)] + [any_spec] * 4,
        out_specs=[any_spec] * 3,
        out_shape=[
            jax.ShapeDtypeStruct(x_loc.shape, bf16),
            jax.ShapeDtypeStruct((rows, cp, n_groups, 2, 2, GROUP, half_len, HEAD_DIM), bf16),
            jax.ShapeDtypeStruct((rows, heads, 2, group_cols // HEAD_DIM, half_len, HEAD_DIM), bf16),
        ],
        scratch_shapes=[
            pltpu.VMEM((2, depth, TILE), bf16),
            pltpu.VMEM((2, ROWS, tok_rows, depth), bf16),
            pltpu.VMEM((2, ROWS, tok_rows, TILE), bf16),
            pltpu.VMEM((toks, TILE), bf16),
            pltpu.VMEM((2, ROWS, fold, 2, GROUP, half_len, HEAD_DIM), bf16),
            pltpu.VMEM((2, toks, inner), bf16),
            pltpu.VMEM((2, ROWS, tok_rows, TILE), bf16),
            pltpu.VMEM((2, 2, group_cols // HEAD_DIM, half_len, HEAD_DIM), bf16),
            pltpu.SemaphoreType.DMA((2,)),
            pltpu.SemaphoreType.DMA((2,)),
            pltpu.SemaphoreType.DMA((2,)),
            pltpu.SemaphoreType.DMA((2,)),
            pltpu.SemaphoreType.DMA((2,)),
            pltpu.SemaphoreType.DMA((2,)),
            pltpu.SemaphoreType.DMA((2,)),
            pltpu.SemaphoreType.DMA((8, 2 * rows)),
            pltpu.SemaphoreType.DMA((8, 2 * rows)),
        ] + attn_scratch(cp, half_len),
        compiler_params=pltpu.CompilerParams(dimension_semantics=('arbitrary',), collective_id=0, has_side_effects=True, vmem_limit_bytes=VMEM_LIMIT),
        cost_estimate=pl.CostEstimate(flops=flops, bytes_accessed=4 * rows * tok_rows * depth, transcendentals=0),
    )(x_loc, cosine, sine, w_query, w_key, w_value, w_out)
    return y


def solution(mesh):
    row_spec, pos_spec, rep_spec = P('data', 'cp', None), P('data', 'cp'), P(None, None)

    def local_block(x_loc, pos_loc, w_query, w_key, w_value, w_out):
        cosine, sine = rope_tables(pos_loc)
        return layer(mesh, x_loc, cosine, sine, w_query, w_key, w_value, w_out)

    return jax.shard_map(local_block, mesh=mesh, in_specs=(row_spec, pos_spec, rep_spec, rep_spec, rep_spec, rep_spec), out_specs=row_spec, check_vma=False)
```

```python
import functools
import math

import jax
import jax.numpy as jnp
from jax import lax
from jax.experimental import pallas as pl
from jax.experimental.pallas import tpu as pltpu
from jax.sharding import PartitionSpec as P

HEAD_DIM = 128
ROPE_BASE = 500000
MASK_FILL = -1e30
EXP_SCALE = float(HEAD_DIM ** -0.5 * math.log2(math.e))
CORES = 2
ROWS = 2
TILE = 1024
GROUP = 4
PAIR = 256
VMEM_LIMIT = 66_000_000
LAG = 5
DELAY = 2
BACK = (2, 0)
EPI = 3
SINGLE = 2
COST = (4.85, 4.72, 1.6, 22.8, 0.3, 1.75, 18.0)
SPLIT = 2
R1, L1, X0, R2, L2, X1, X2, X3 = range(8)
f32, bf16 = jnp.float32, jnp.bfloat16
div, rem = lax.div, lax.rem


def rope_tables(positions):
    half = HEAD_DIM // 2
    inv_freq = 1.0 / (ROPE_BASE ** (jnp.arange(0, HEAD_DIM, 2, dtype=f32) / HEAD_DIM))
    half_len = positions.shape[1] // 2
    pos = positions.astype(f32)
    front = jnp.broadcast_to(pos[:, :half_len, None], pos[:, :half_len].shape + (half,))
    back = jnp.broadcast_to(pos[:, half_len:, None], front.shape)
    angles = (jnp.concatenate([front, back], axis=-1) * jnp.concatenate([inv_freq, inv_freq])).reshape(-1, HEAD_DIM)
    return jnp.cos(angles), jnp.sin(angles)


def attn_steps(cp):
    dyn = cp // 2 - 1
    return ['front'] + ['extra'] + [('pair', k) for k in range(dyn)] + ['back'] + [('pair', k) for k in range(dyn, cp - 1)]


def attn_scratch(cp, half_len):
    steps = attn_steps(cp)
    blocks = sum(1 if isinstance(t, str) else 2 for t in steps)
    groups = lambda *shape: [pltpu.VMEM(shape, f32), pltpu.VMEM(shape, f32)]
    return [
        pltpu.VMEM((2, cp, 2, 2, GROUP, HEAD_DIM, half_len), bf16),
        *groups(blocks * half_len, PAIR),
        *groups(1 + len(BACK), HEAD_DIM, PAIR),
        *groups(cp // 2 + 1, HEAD_DIM, PAIR),
        *groups(2, 1, PAIR),
        *groups(2, 1, PAIR),
        pltpu.VMEM((half_len, half_len), f32),
    ]


def attn_init(cp, scratch):
    _, _, _, _, _, pv0, pv1, _, _, _, _, bias = scratch
    kpos = lax.broadcasted_iota(jnp.int32, bias.shape, 0)
    qpos = lax.broadcasted_iota(jnp.int32, bias.shape, 1)
    for ref in (pv0, pv1):
        ref[ref.shape[0] - 1] = jnp.zeros(ref.shape[1:], f32)
    bias[...] = jnp.where(kpos <= qpos, 0.0, MASK_FILL)


def attn_step(n, cp, my, q_ref, put, scratch):
    kvbuf, sc0, sc1, ac0, ac1, pv0, pv1, mx0, mx1, sm0, sm1, bias = scratch
    sbuf, acc, pvb, mst, lst = (sc0, sc1), (ac0, ac1), (pv0, pv1), (mx0, mx1), (sm0, sm1)
    steps, parts = attn_steps(cp), cp // 2
    half_len = kvbuf.shape[6]
    here = (rem(div(n, GROUP), 2), rem(n, GROUP))
    before = jnp.maximum(n - 1, 0)
    behind_ = (rem(div(before, GROUP), 2), rem(before, GROUP))
    pairs, par = div(my, 2), rem(my, 2)

    def place(j):
        front = j < cp
        return jnp.where(front, j, 2 * cp - 1 - j), jnp.where(front, 0, 1)

    front_of, part_of, locs, rows_of, row = {}, {}, {}, {}, 0
    for t in steps:
        if t == 'front':
            front_of[t], blocks = True, [my]
        elif t == 'back':
            front_of[t], blocks = False, [2 * cp - 1 - my]
        elif t == 'extra':
            front_of[t], part_of[t], blocks = par == 1, 0, [jnp.where(par == 1, my - 1, 2 * cp - 2 - my)]
        else:
            k = t[1]
            if k < parts - 1:
                front_of[t], part_of[t] = k < pairs, 1 + k
                first = 2 * jnp.where(k < pairs, k, k - pairs)
            else:
                front_of[t], first = False, 2 * (k - pairs)
            blocks = [first, first + 1]
        locs[t] = [place(j) for j in blocks]
        rows_of[t] = slice(row, row + len(blocks) * half_len)
        row += len(blocks) * half_len
    low = jnp.full((1, PAIR), MASK_FILL, f32)
    zero = jnp.zeros((1, PAIR), f32)

    def half_of(t):
        return jnp.where(front_of[t], 0, 1) if t in part_of else 0 if front_of[t] else 1

    def stack(items, axis):
        return items[0] if len(items) == 1 else jnp.concatenate(items, axis=axis)

    def scores(t, g):
        slot, e = here
        k = stack([kvbuf[slot, s, 0, f, e] for s, f in locs[t]], 0)
        s = lax.dot_general(k, q_ref[half_of(t), 2 * g:2 * g + 2].reshape(PAIR, HEAD_DIM), (((1,), (1,)), ((), ())), preferred_element_type=f32)
        if t in ('front', 'back'):
            b = bias[...]
            s = s + jnp.concatenate([b, b], axis=1)
        sbuf[g][rows_of[t]] = s
        return jnp.max(s, axis=0, keepdims=True)

    def finish_max(g, ms):
        front_max, back_max = low, low
        for t, m in zip(steps, ms):
            if t in part_of:
                front_max = jnp.maximum(front_max, jnp.where(front_of[t], m, low))
                back_max = jnp.maximum(back_max, jnp.where(front_of[t], low, m))
            elif front_of[t]:
                front_max = jnp.maximum(front_max, m)
            else:
                back_max = jnp.maximum(back_max, m)
        mst[g][0] = front_max
        mst[g][1] = back_max

    def soft(t, g, behind):
        m = mst[g][half_of(t)]
        if behind is not None:
            m = jnp.maximum(m, jnp.minimum(behind, MASK_FILL))
        p = jnp.exp2((sbuf[g][rows_of[t]] - m) * EXP_SCALE)
        return jnp.sum(p, axis=0, keepdims=True), p.astype(bf16)

    def put_weighted(g, ts, ps, at):
        slot, e = at
        vals = stack([kvbuf[slot, s, 1, f, e] for t in ts for s, f in locs[t]], 1)
        out = lax.dot_general(vals, stack(ps, 0), (((1,), (0,)), ((), ())), preferred_element_type=f32)
        if ts[0] in part_of:
            pvb[g][part_of[ts[0]]] = out
        elif front_of[ts[0]]:
            acc[g][0] = out
        else:
            acc[g][1 + BACK.index(len(steps) - 1 - steps.index(ts[-1]))] = out

    def epilogue(g):
        for half in range(2):
            inv = 1.0 / lst[g][half]
            for e in range(PAIR // HEAD_DIM):
                lanes = slice(e * half_len, (e + 1) * half_len)
                o = acc[g][half, :, lanes]
                for i in range(1, len(BACK) if half else 1):
                    o = o + acc[g][1 + i, :, lanes]
                for t, part in part_of.items():
                    mine = front_of[t] if half == 0 else jnp.logical_not(front_of[t])
                    o = o + pvb[g][jnp.where(mine, part, parts), :, lanes]
                put(half, g * (PAIR // HEAD_DIM) + e, (o * inv[:, lanes]).astype(bf16).T)
                yield

    pending = []

    def drain(limit):
        while len(pending) > limit:
            put_weighted(*pending.pop(0))

    for g1, g2, at in ((0, 1, behind_), (1, 0, here)):
        epi = epilogue(g1)
        ms, front_sum, back_sum, held = [], zero, zero, []
        for i, t in enumerate(steps):
            ms.append(scores(t, g1))
            l, p = soft(t, g2, ms[i - LAG] if i >= LAG else None)
            if t in part_of:
                front_sum = front_sum + jnp.where(front_of[t], l, zero)
                back_sum = back_sum + jnp.where(front_of[t], zero, l)
            elif front_of[t]:
                front_sum = front_sum + l
            else:
                back_sum = back_sum + l
            if t in part_of or front_of[t]:
                pending.append((g2, [t], [p], at))
            else:
                held.append((t, p))
                if len(steps) - 1 - i in BACK:
                    pending.append((g2, [t for t, _ in held], [p for _, p in held], at))
                    held = []
            drain(DELAY)
            if i >= EPI:
                next(epi, None)
        lst[g2][0] = front_sum
        lst[g2][1] = back_sum
        finish_max(g1, ms)
        for _ in epi:
            pass
    drain(0)


def plan_steps(chunks, n_proj, n_out, per_chunk, send_at):
    half = per_chunk // 2
    seq = [('P', i) for i in range(chunks * n_proj)] + [('F', 0)]
    for c in range(chunks):
        seq += [('A', c * per_chunk + i) for i in range(half)]
        if c:
            seq += [('O', (c - 1) * n_out + i) for i in range(n_out)]
        seq += [('A', c * per_chunk + i) for i in range(half, per_chunk)]
    seq += [('S', chunks * per_chunk)] + [('O', (chunks - 1) * n_out + i) for i in range(n_out)]
    units = [(c * ROWS, ROWS) for c in range(chunks - SINGLE)] + [(i, 1) for i in range((chunks - SINGLE) * ROWS, chunks * ROWS)]
    first_use = [seq.index(('A', row * per_chunk // ROWS)) for row, _ in units]
    proj, out, att, wire, pause, inner, now = COST
    took = {'P': proj, 'O': out, 'A': att, 'S': att, 'F': 0.6}
    hops = {'one': [], 'two': [], 'three': [], 'in': []}
    link, core, got1, got2, sent = 0.0, 0.0, {}, {}, -1
    for step, (kind, i) in enumerate(seq):
        if step and seq[step - 1][0] == 'P' and seq[step - 1][1] % n_proj == send_at:
            sent = seq[step - 1][1] // n_proj
        must = max((u for u in range(len(units)) if first_use[u] <= step + 1), default=-1)
        done = lambda name: len(hops[name])
        while done('one') < len(units) or done('two') < len(units):
            u = done('two')
            if done('one') < min(u + 2, len(units)):
                u = done('one')
                if units[u][0] // ROWS > sent:
                    break
                link = max(now, link) + wire * units[u][1] + pause
                got1[u] = link
                hops['one'].append(step)
            else:
                if now < got1[u] + 3 and u > must:
                    break
                now = max(now, got1[u])
                link = max(now, link) + wire * units[u][1] / 2 + pause
                core = max(now, core) + 2 * inner * units[u][1]
                got2[u] = max(link, core)
                hops['two'].append(step)
        while done('three') < done('two') and (got2[done('three')] + 3 <= now or done('three') <= must):
            u = done('three')
            now = max(now, got2[u])
            core = max(now, core) + inner * units[u][1]
            hops['three'].append(step)
        now += took[kind]
    for u in range(len(units)):
        hops['in'].append(first_use[u] - 1)
    return seq, units, hops


def layer(mesh, x_loc, cosine, sine, w_query, w_key, w_value, w_out):
    cp = mesh.shape['cp']
    rows, tok_rows, depth = x_loc.shape
    half_len = tok_rows // 2
    inner, kv_cols = w_query.shape[1], w_key.shape[1]
    heads = kv_cols // HEAD_DIM
    group_cols = inner // heads
    per_tile, fold = TILE // HEAD_DIM, TILE // HEAD_DIM // GROUP
    toks = ROWS * tok_rows
    chunks = rows // ROWS
    kt, qt, n_out = kv_cols // TILE, inner // TILE, depth // TILE
    n_proj = 2 * kt + qt
    per_chunk = ROWS * heads
    total = rows * heads
    n_groups = heads // GROUP
    assert n_groups == 2
    assert depth == w_query.shape[0] and group_cols == 2 * PAIR and rows % ROWS == 0
    assert kt == 1 and n_proj > 4 and group_cols == GROUP * HEAD_DIM and cp // CORES == 4
    seq, units, hops = plan_steps(chunks, n_proj, n_out, per_chunk, 2 * kt)
    n_steps = len(seq)
    half_chunk, period = per_chunk // 2, per_chunk + n_out
    all_proj = n_proj * chunks
    first_a, second_a, last_a = (seq.index(('A', 0)), seq.index(('A', per_chunk)), seq.index(('S', total)))
    n_tiles = (n_proj + n_out) * chunks

    def pick(cases, other):
        for cond, val in reversed(cases):
            other = jnp.where(cond, val, other)
        return other

    def kern(x_hbm, cos_ref, sin_ref, wq_hbm, wk_hbm, wv_hbm, wo_hbm, y_hbm, kv_hbm, q_hbm,
             wbuf, xbuf, xres, raw, stage, oscr, ybuf, qbuf,
             wsem, xsem, rsem, osem, ysem, qsem, kvsem, send_sem, recv_sem, *attn):
        s = pl.program_id(0)
        my = lax.axis_index('cp')
        chip, core = div(my, CORES), rem(my, CORES)
        chips = cp // CORES

        def device(chip_shift, core_shift=0):
            return rem(chip + chip_shift, chips) * CORES + rem(core + core_shift, CORES)

        nxt, far, prv, mate = device(1), device(2), device(chips - 1), device(0, 1)

        a, r = 1 + div(s - second_a, period), rem(s - second_a, period)
        is_proj, is_flush = s < all_proj, s == all_proj
        in_first, is_skew = s < second_a, s == last_a
        past = jnp.where(s > last_a, period, 0)
        is_out = jnp.logical_or(past > 0, jnp.logical_and(jnp.logical_not(in_first), jnp.logical_and(r >= half_chunk, r < half_chunk + n_out)))
        is_head = jnp.logical_and(s > all_proj, jnp.logical_not(is_out))
        is_new = jnp.logical_and(is_head, jnp.logical_not(is_skew))
        n = jnp.where(in_first, s - first_a, a * per_chunk + jnp.where(r >= half_chunk + n_out, r - n_out, r))
        oidx = jnp.where(past > 0, s - last_a - 1 + (chunks - 1) * n_out, (a - 1) * n_out + r - half_chunk)
        pidx = s
        oc, col = div(oidx, n_out), rem(oidx, n_out)
        pc, pt = div(pidx, n_proj), rem(pidx, n_proj)
        tile_p, tile_o = pidx, all_proj + oidx

        def row_ds(c):
            return pl.ds(c * ROWS, ROWS)

        def load_tile(j):
            slot = rem(j, 2)
            is_p = j < all_proj
            p = rem(j, n_proj)
            o_chunk, o_col = div(j - all_proj, n_out), rem(j - all_proj, n_out)

            def start(w_hbm, tile_col):
                cols = pl.ds(pl.multiple_of(tile_col * TILE, TILE), TILE)
                part = w_hbm.shape[0] // SPLIT
                for i in range(SPLIT):
                    ks = pl.ds(i * part, part)
                    pltpu.make_async_copy(w_hbm.at[ks, cols], wbuf.at[slot, ks], wsem.at[slot]).start()

            @pl.when(jnp.logical_and(is_p, p < kt))
            def _():
                start(wk_hbm, p)

            @pl.when(jnp.logical_and(is_p, jnp.logical_and(p >= kt, p < 2 * kt)))
            def _():
                start(wv_hbm, p - kt)

            @pl.when(jnp.logical_and(is_p, p >= 2 * kt))
            def _():
                start(wq_hbm, p - 2 * kt)

            @pl.when(jnp.logical_not(is_p))
            def _():
                start(wo_hbm, o_col)
                load_res(o_chunk, o_col, slot).start()

        def load_res(c, tile_col, slot):
            cols = pl.ds(pl.multiple_of(tile_col * TILE, TILE), TILE)
            return pltpu.make_async_copy(x_hbm.at[row_ds(c), :, cols], xres.at[slot], rsem.at[slot])

        def next_tile(j):
            @pl.when(j + 1 < n_tiles)
            def _():
                load_tile(j + 1)
            slot = rem(j, 2)
            pltpu.make_async_copy(wo_hbm.at[:, pl.ds(0, TILE)], wbuf.at[slot], wsem.at[slot]).wait()
            return slot

        def load_x(c):
            return pltpu.make_async_copy(x_hbm.at[row_ds(c)], xbuf.at[rem(c, 2)], xsem.at[rem(c, 2)])

        def load_q(m):
            return pltpu.make_async_copy(q_hbm.at[div(m, heads), rem(m, heads)], qbuf.at[rem(m, 2)], qsem.at[rem(m, 2)])

        def load_kv(g):
            slot = rem(g, 2)
            return [pltpu.make_async_copy(kv_hbm.at[div(g, n_groups), src, rem(g, n_groups)], attn[0].at[slot, src], kvsem.at[slot]) for src in range(cp)]

        def wait_kv(g):
            slot = rem(g, 2)
            pltpu.make_async_copy(kv_hbm.at[0, :, 0], attn[0].at[slot], kvsem.at[slot]).wait()

        def store_y(c, tile_col, slot):
            cols = pl.ds(pl.multiple_of(tile_col * TILE, TILE), TILE)
            return pltpu.make_async_copy(ybuf.at[slot], y_hbm.at[row_ds(c), :, cols], ysem.at[slot])

        def hop(kind, row, size, only=None, sem=0):
            rs = pl.ds(row, size)
            src, to = {R1: (my, nxt), L1: (my, prv), X0: (my, mate), R2: (prv, nxt), L2: (nxt, prv), X1: (nxt, mate), X2: (far, mate), X3: (prv, mate)}[kind]
            if kind in (R2, L2):
                ref = kv_hbm.at[rs, src, 0 if kind == R2 else 1]
            else:
                ref = kv_hbm.at[rs, src] if only is None else kv_hbm.at[rs, src, :, only]
            sem = 2 * row if only is None else sem
            return pltpu.make_async_remote_copy(src_ref=ref, dst_ref=ref, send_sem=send_sem.at[kind, sem], recv_sem=recv_sem.at[kind, sem],
                                                device_id={'cp': to}, device_id_type=pl.DeviceIdType.MESH)

        def first_copies(only, act):
            @pl.when(core == 0)
            def _():
                for kind in (R1, L1):
                    act(hop(kind, 0, ROWS, only, only))

            @pl.when(core != 0)
            def _():
                for kind in (R1, L1):
                    for i in range(ROWS):
                        act(hop(kind, i, 1, only, ROWS * only + i))

        def ring_one(row, size, act, parts=(0, 1)):
            @pl.when(row == 0)
            def _():
                for only in parts:
                    first_copies(only, act)

            @pl.when(row != 0)
            def _():
                near((R1, L1), row, size, act)

        def near(kinds, row, size, act):
            @pl.when(size == 1)
            def _():
                for kind in kinds:
                    act(hop(kind, row, 1))

            @pl.when(size != 1)
            def _():
                for kind in kinds:
                    act(hop(kind, row, ROWS))

        start, received, left = (lambda c: c.start()), (lambda c: c.wait_recv()), (lambda c: c.wait_send())

        def hop_one(row, size):
            ring_one(row, size, start, (1,))
            near((X0,), row, size, start)

        def hop_two(row, size):
            ring_one(row, size, received)
            near((R2, L2, X1, X3), row, size, start)

        def hop_three(row, size):
            near((R2, L2), row, size, received)
            near((X2,), row, size, start)

        def arrive(row, size):
            near((X0, X1, X3, X2), row, size, received)
            ring_one(row, size, left)
            near((R2, L2, X0, X1, X3, X2), row, size, left)
            for copy in load_kv(row * n_groups):
                copy.start()

            @pl.when(row == 0)
            def _():
                load_q(0).start()

        def unit_hops(lo, hi):
            for name, act in (('two', hop_two), ('one', hop_one), ('three', hop_three), ('in', arrive)):
                due = [(step, units[u]) for u, step in enumerate(hops[name]) if lo <= step < hi]
                if not due:
                    continue
                row, size = pick([(s == step, row) for step, (row, _) in due], -1), pick([(s == step, size) for step, (_, size) in due], ROWS)

                @pl.when(row >= 0)
                def _(row=row, size=size, act=act):
                    act(row, size)

        @pl.when(s == 0)
        def _():
            barrier = pltpu.get_barrier_semaphore()
            for to in (nxt, prv, mate):
                pl.semaphore_signal(barrier, inc=1, device_id={'cp': to}, device_id_type=pl.DeviceIdType.MESH)
            load_x(0).start()
            load_tile(0)
            attn_init(cp, attn)
            pl.semaphore_wait(barrier, 3)

        def store_tile(p):
            c, tile, slot = div(p, n_proj), rem(p, n_proj), rem(p, 2)
            rs = row_ds(c)

            @pl.when(tile < 2)
            def _():
                pltpu.make_async_copy(stage.at[slot], kv_hbm.at[rs, my, :, tile], osem.at[slot]).start()

            @pl.when(tile >= 2)
            def _():
                pltpu.make_async_copy(stage.at[slot], q_hbm.at[rs, pl.ds((tile - 2) * fold, fold)], osem.at[slot]).start()

        def wait_store(p):
            slot = rem(p, 2)
            pltpu.make_async_copy(stage.at[slot], q_hbm.at[pl.ds(0, ROWS), pl.ds(0, fold)], osem.at[slot]).wait()

        def rope_epilogue(p):
            c, slot = div(p, n_proj), rem(p, 2)
            is_v = rem(p, n_proj) == 1
            low_lanes = lax.broadcasted_iota(jnp.int32, (half_len, HEAD_DIM), 1) < HEAD_DIM // 2
            for i in range(ROWS):
                ts = pl.ds(pl.multiple_of((c * ROWS + i) * half_len, half_len), half_len)
                cos, sin = cos_ref[ts], sin_ref[ts]
                cos_r, sin_r = pltpu.roll(cos, HEAD_DIM // 2, 1), pltpu.roll(sin, HEAD_DIM // 2, 1)
                for half in range(2):
                    cos_h = jnp.where(low_lanes, cos, cos_r) if half == 0 else jnp.where(low_lanes, cos_r, cos)
                    sin_h = jnp.where(low_lanes, -sin, sin_r) if half == 0 else jnp.where(low_lanes, -sin_r, sin)
                    rs = slice(i * tok_rows + half * half_len, i * tok_rows + (half + 1) * half_len)
                    for e in range(per_tile):
                        vals = raw[rs, e * HEAD_DIM:(e + 1) * HEAD_DIM]
                        wide = vals.astype(f32)
                        turned = (wide * cos_h + pltpu.roll(wide, HEAD_DIM // 2, 1) * sin_h).astype(bf16)
                        stage[slot, i, e // GROUP, half, e % GROUP] = jnp.where(is_v, vals.T, turned)

        @pl.when(is_proj)
        def _():
            next_tile(tile_p)

            @pl.when(jnp.logical_and(pidx > 3, pt != 4))
            def _():
                wait_store(pidx - 3)

            @pl.when(pidx == 2)
            def _():
                wait_store(0)
                first_copies(0, start)

            @pl.when(pt == 3)
            def _():
                wait_store(pidx - 2)

            @pl.when(pt == 0)
            def _():
                load_x(pc).wait()

            @pl.when(jnp.logical_and(pt == 1, pc + 1 < chunks))
            def _():
                load_x(pc + 1).start()

        spans = 6
        for i in range(spans):
            lo, hi = n_steps * i // spans, n_steps * (i + 1) // spans

            @pl.when(jnp.logical_and(s >= lo, s < hi))
            def _(lo=lo, hi=hi):
                unit_hops(lo, hi)

        @pl.when(is_proj)
        def _():
            rope_epilogue(jnp.maximum(pidx - 1, 0))
            x = xbuf[rem(pc, 2)].reshape(toks, depth)
            raw[...] = jnp.dot(x, wbuf[rem(tile_p, 2)], preferred_element_type=f32).astype(bf16)

            @pl.when(pidx >= 1)
            def _():
                store_tile(pidx - 1)

        @pl.when(is_flush)
        def _():
            end = n_proj * chunks
            wait_store(end - 3)
            rope_epilogue(end - 1)
            store_tile(end - 1)
            wait_store(end - 2)
            wait_store(end - 1)

        @pl.when(is_head)
        def _():
            g = div(n, GROUP)

            @pl.when(is_new)
            def _():
                load_q(n).wait()

                @pl.when(n + 1 < total)
                def _():
                    load_q(n + 1).start()

                @pl.when(rem(n, GROUP) == 0)
                def _():
                    wait_kv(g)

                fresh = jnp.logical_or(rem(g + 1, ROWS * n_groups) == 0, jnp.logical_and(g + 1 >= (rows - SINGLE * ROWS) * n_groups, rem(g + 1, n_groups) == 0))

                @pl.when(jnp.logical_and(rem(n, GROUP) == 1, jnp.logical_not(fresh)))
                def _():
                    for copy in load_kv(g + 1):
                        copy.start()

            m = jnp.maximum(n - 1, 0)
            o_slot = rem(div(m, per_chunk), 2)
            row, head = rem(div(m, heads), ROWS), rem(m, heads)

            def put(half, j, val):
                rs = pl.ds(pl.multiple_of(row * tok_rows + half * half_len, half_len), half_len)
                cs = pl.ds(pl.multiple_of(head * group_cols + j * HEAD_DIM, HEAD_DIM), HEAD_DIM)
                oscr[o_slot, rs, cs] = val

            attn_step(n, cp, my, qbuf.at[rem(n, 2)], put, attn)

        @pl.when(is_out)
        def _():
            slot = next_tile(tile_o)
            y_slot = rem(oidx, 2)
            load_res(oc, col, slot).wait()

            @pl.when(oidx >= 2)
            def _():
                store_y(0, 0, y_slot).wait()

            out = jnp.dot(oscr[rem(oc, 2)], wbuf[slot], preferred_element_type=f32)
            ybuf[y_slot] = (xres[slot].astype(f32) + out.reshape(ROWS, tok_rows, TILE)).astype(bf16)
            store_y(oc, col, y_slot).start()

            @pl.when(oidx == n_out * chunks - 1)
            def _():
                store_y(0, 0, 1 - y_slot).wait()
                store_y(0, 0, y_slot).wait()

    any_spec = pl.BlockSpec(memory_space=pl.ANY)
    flops = 2 * rows * tok_rows * depth * (2 * inner + 2 * kv_cols) + 8 * total * (cp + 1) * half_len * group_cols * HEAD_DIM * 2
    y, _, _ = pl.pallas_call(
        kern,
        name='layer',
        grid=(n_steps,),
        in_specs=[any_spec, pl.BlockSpec(memory_space=pltpu.VMEM), pl.BlockSpec(memory_space=pltpu.VMEM)] + [any_spec] * 4,
        out_specs=[any_spec] * 3,
        out_shape=[
            jax.ShapeDtypeStruct(x_loc.shape, bf16),
            jax.ShapeDtypeStruct((rows, cp, n_groups, 2, 2, GROUP, half_len, HEAD_DIM), bf16),
            jax.ShapeDtypeStruct((rows, heads, 2, group_cols // HEAD_DIM, half_len, HEAD_DIM), bf16),
        ],
        scratch_shapes=[
            pltpu.VMEM((2, depth, TILE), bf16),
            pltpu.VMEM((2, ROWS, tok_rows, depth), bf16),
            pltpu.VMEM((2, ROWS, tok_rows, TILE), bf16),
            pltpu.VMEM((toks, TILE), bf16),
            pltpu.VMEM((2, ROWS, fold, 2, GROUP, half_len, HEAD_DIM), bf16),
            pltpu.VMEM((2, toks, inner), bf16),
            pltpu.VMEM((2, ROWS, tok_rows, TILE), bf16),
            pltpu.VMEM((2, 2, group_cols // HEAD_DIM, half_len, HEAD_DIM), bf16),
            pltpu.SemaphoreType.DMA((2,)),
            pltpu.SemaphoreType.DMA((2,)),
            pltpu.SemaphoreType.DMA((2,)),
            pltpu.SemaphoreType.DMA((2,)),
            pltpu.SemaphoreType.DMA((2,)),
            pltpu.SemaphoreType.DMA((2,)),
            pltpu.SemaphoreType.DMA((2,)),
            pltpu.SemaphoreType.DMA((8, 2 * rows)),
            pltpu.SemaphoreType.DMA((8, 2 * rows)),
        ] + attn_scratch(cp, half_len),
        compiler_params=pltpu.CompilerParams(dimension_semantics=('arbitrary',), collective_id=0, has_side_effects=True, vmem_limit_bytes=VMEM_LIMIT),
        cost_estimate=pl.CostEstimate(flops=flops, bytes_accessed=4 * rows * tok_rows * depth, transcendentals=0),
    )(x_loc, cosine, sine, w_query, w_key, w_value, w_out)
    return y


def solution(mesh):
    row_spec, pos_spec, rep_spec = P('data', 'cp', None), P('data', 'cp'), P(None, None)

    def local_block(x_loc, pos_loc, w_query, w_key, w_value, w_out):
        cosine, sine = rope_tables(pos_loc)
        return layer(mesh, x_loc, cosine, sine, w_query, w_key, w_value, w_out)

    return jax.shard_map(local_block, mesh=mesh, in_specs=(row_spec, pos_spec, rep_spec, rep_spec, rep_spec, rep_spec), out_specs=row_spec, check_vma=False)
```

```python
import functools
import math

import jax
import jax.numpy as jnp
from jax import lax
from jax.experimental import pallas as pl
from jax.experimental.pallas import tpu as pltpu
from jax.sharding import PartitionSpec as P

HEAD_DIM = 128
ROPE_BASE = 500000
MASK_FILL = -1e30
EXP_SCALE = float(HEAD_DIM ** -0.5 * math.log2(math.e))
CORES = 2
ROWS = 2
TILE = 1024
GROUP = 4
STEP_HEADS = 2
PAIR = 256
VMEM_LIMIT = 66_000_000
LAG = 5
DELAY = 2
BACK = (2, 0)
EPI = 3
SINGLE = 2
COST = (4.85, 4.72, 2.95, 22.8, 0.4, 1.75, 18.0)
SLACK = 0.3
SPLIT = 4
R1, L1, X0, R2, L2, X1, X2, X3 = range(8)
f32, bf16 = jnp.float32, jnp.bfloat16
div, rem = lax.div, lax.rem


def rope_tables(positions):
    half = HEAD_DIM // 2
    inv_freq = 1.0 / (ROPE_BASE ** (jnp.arange(0, HEAD_DIM, 2, dtype=f32) / HEAD_DIM))
    half_len = positions.shape[1] // 2
    pos = positions.astype(f32)
    front = jnp.broadcast_to(pos[:, :half_len, None], pos[:, :half_len].shape + (half,))
    back = jnp.broadcast_to(pos[:, half_len:, None], front.shape)
    angles = (jnp.concatenate([front, back], axis=-1) * jnp.concatenate([inv_freq, inv_freq])).reshape(-1, HEAD_DIM)
    return jnp.cos(angles), jnp.sin(angles)


def attn_steps(cp):
    dyn = cp // 2 - 1
    return ['front'] + ['extra'] + [('pair', k) for k in range(dyn)] + ['back'] + [('pair', k) for k in range(dyn, cp - 1)]


def attn_scratch(cp, half_len):
    steps = attn_steps(cp)
    blocks = sum(1 if isinstance(t, str) else 2 for t in steps)
    groups = lambda *shape: [pltpu.VMEM(shape, f32), pltpu.VMEM(shape, f32)]
    return [
        pltpu.VMEM((2, cp, 2, 2, GROUP, HEAD_DIM, half_len), bf16),
        *groups(blocks * half_len, PAIR),
        *groups(1 + len(BACK), HEAD_DIM, PAIR),
        *groups(cp // 2 + 1, HEAD_DIM, PAIR),
        *groups(2, 1, PAIR),
        *groups(2, 1, PAIR),
        pltpu.VMEM((half_len, half_len), f32),
    ]


def attn_init(cp, scratch):
    _, _, _, _, _, pv0, pv1, _, _, _, _, bias = scratch
    kpos = lax.broadcasted_iota(jnp.int32, bias.shape, 0)
    qpos = lax.broadcasted_iota(jnp.int32, bias.shape, 1)
    for ref in (pv0, pv1):
        ref[ref.shape[0] - 1] = jnp.zeros(ref.shape[1:], f32)
    bias[...] = jnp.where(kpos <= qpos, 0.0, MASK_FILL)


def attn_step(n, cp, my, q_ref, put, scratch):
    kvbuf, sc0, sc1, ac0, ac1, pv0, pv1, mx0, mx1, sm0, sm1, bias = scratch
    sbuf, acc, pvb, mst, lst = (sc0, sc1), (ac0, ac1), (pv0, pv1), (mx0, mx1), (sm0, sm1)
    steps, parts = attn_steps(cp), cp // 2
    half_len = kvbuf.shape[6]
    here = (rem(div(n, GROUP), 2), rem(n, GROUP))
    before = jnp.maximum(n - 1, 0)
    behind_ = (rem(div(before, GROUP), 2), rem(before, GROUP))
    pairs, par = div(my, 2), rem(my, 2)

    def place(j):
        front = j < cp
        return jnp.where(front, j, 2 * cp - 1 - j), jnp.where(front, 0, 1)

    front_of, part_of, locs, rows_of, row = {}, {}, {}, {}, 0
    for t in steps:
        if t == 'front':
            front_of[t], blocks = True, [my]
        elif t == 'back':
            front_of[t], blocks = False, [2 * cp - 1 - my]
        elif t == 'extra':
            front_of[t], part_of[t], blocks = par == 1, 0, [jnp.where(par == 1, my - 1, 2 * cp - 2 - my)]
        else:
            k = t[1]
            if k < parts - 1:
                front_of[t], part_of[t] = k < pairs, 1 + k
                first = 2 * jnp.where(k < pairs, k, k - pairs)
            else:
                front_of[t], first = False, 2 * (k - pairs)
            blocks = [first, first + 1]
        locs[t] = [place(j) for j in blocks]
        rows_of[t] = slice(row, row + len(blocks) * half_len)
        row += len(blocks) * half_len
    low = jnp.full((1, PAIR), MASK_FILL, f32)
    zero = jnp.zeros((1, PAIR), f32)

    def half_of(t):
        return jnp.where(front_of[t], 0, 1) if t in part_of else 0 if front_of[t] else 1

    def stack(items, axis):
        return items[0] if len(items) == 1 else jnp.concatenate(items, axis=axis)

    def scores(t, g):
        slot, e = here
        k = stack([kvbuf[slot, s, 0, f, e] for s, f in locs[t]], 0)
        s = lax.dot_general(k, q_ref[half_of(t), 2 * g:2 * g + 2].reshape(PAIR, HEAD_DIM), (((1,), (1,)), ((), ())), preferred_element_type=f32)
        if t in ('front', 'back'):
            b = bias[...]
            s = s + jnp.concatenate([b, b], axis=1)
        sbuf[g][rows_of[t]] = s
        return jnp.max(s, axis=0, keepdims=True)

    def finish_max(g, ms):
        front_max, back_max = low, low
        for t, m in zip(steps, ms):
            if t in part_of:
                front_max = jnp.maximum(front_max, jnp.where(front_of[t], m, low))
                back_max = jnp.maximum(back_max, jnp.where(front_of[t], low, m))
            elif front_of[t]:
                front_max = jnp.maximum(front_max, m)
            else:
                back_max = jnp.maximum(back_max, m)
        mst[g][0] = front_max
        mst[g][1] = back_max

    def soft(t, g, behind):
        m = mst[g][half_of(t)]
        if behind is not None:
            m = jnp.maximum(m, jnp.minimum(behind, MASK_FILL))
        p = jnp.exp2((sbuf[g][rows_of[t]] - m) * EXP_SCALE)
        return jnp.sum(p, axis=0, keepdims=True), p.astype(bf16)

    def put_weighted(g, ts, ps, at):
        slot, e = at
        vals = stack([kvbuf[slot, s, 1, f, e] for t in ts for s, f in locs[t]], 1)
        out = lax.dot_general(vals, stack(ps, 0), (((1,), (0,)), ((), ())), preferred_element_type=f32)
        if ts[0] in part_of:
            pvb[g][part_of[ts[0]]] = out
        elif front_of[ts[0]]:
            acc[g][0] = out
        else:
            acc[g][1 + BACK.index(len(steps) - 1 - steps.index(ts[-1]))] = out

    def epilogue(g):
        for half in range(2):
            inv = 1.0 / lst[g][half]
            for e in range(PAIR // HEAD_DIM):
                lanes = slice(e * half_len, (e + 1) * half_len)
                o = acc[g][half, :, lanes]
                for i in range(1, len(BACK) if half else 1):
                    o = o + acc[g][1 + i, :, lanes]
                for t, part in part_of.items():
                    mine = front_of[t] if half == 0 else jnp.logical_not(front_of[t])
                    o = o + pvb[g][jnp.where(mine, part, parts), :, lanes]
                put(half, g * (PAIR // HEAD_DIM) + e, (o * inv[:, lanes]).astype(bf16).T)
                yield

    pending = []

    def drain(limit):
        while len(pending) > limit:
            put_weighted(*pending.pop(0))

    for g1, g2, at in ((0, 1, behind_), (1, 0, here)):
        epi = epilogue(g1)
        ms, front_sum, back_sum, held = [], zero, zero, []
        for i, t in enumerate(steps):
            ms.append(scores(t, g1))
            l, p = soft(t, g2, ms[i - LAG] if i >= LAG else None)
            if t in part_of:
                front_sum = front_sum + jnp.where(front_of[t], l, zero)
                back_sum = back_sum + jnp.where(front_of[t], zero, l)
            elif front_of[t]:
                front_sum = front_sum + l
            else:
                back_sum = back_sum + l
            if t in part_of or front_of[t]:
                pending.append((g2, [t], [p], at))
            else:
                held.append((t, p))
                if len(steps) - 1 - i in BACK:
                    pending.append((g2, [t for t, _ in held], [p for _, p in held], at))
                    held = []
            drain(DELAY)
            if i >= EPI:
                next(epi, None)
        lst[g2][0] = front_sum
        lst[g2][1] = back_sum
        finish_max(g1, ms)
        for _ in epi:
            pass
    drain(0)


def plan_steps(chunks, n_proj, n_out, per_chunk, send_at):
    half = per_chunk // 2
    seq = [('P', i) for i in range(chunks * n_proj)] + [('F', 0)]
    for c in range(chunks):
        seq += [('A', c * per_chunk + i) for i in range(half)]
        if c:
            seq += [('O', (c - 1) * n_out + i) for i in range(n_out)]
        seq += [('A', c * per_chunk + i) for i in range(half, per_chunk)]
    seq += [('S', chunks * per_chunk)] + [('O', (chunks - 1) * n_out + i) for i in range(n_out)]
    units = [(c * ROWS, ROWS) for c in range(chunks - SINGLE)] + [(i, 1) for i in range((chunks - SINGLE) * ROWS, chunks * ROWS)]
    first_use = [seq.index(('A', row * per_chunk // ROWS)) for row, _ in units]
    proj, out, att, wire, pause, inner, now = COST
    took = {'P': proj, 'O': out, 'A': att, 'S': att, 'F': 0.6}
    amount = lambda u: units[u][1]
    hops = {'one': [], 'two': [], 'three': [], 'in': []}
    link, core, got1, got2, sent = 0.0, 0.0, {}, {}, -1
    for step, (kind, i) in enumerate(seq):
        if step and seq[step - 1][0] == 'P' and seq[step - 1][1] % n_proj == send_at:
            sent = seq[step - 1][1] // n_proj
        must = max((u for u in range(len(units)) if first_use[u] <= step + 1), default=-1)
        done = lambda name: len(hops[name])
        while done('one') < len(units) or done('two') < len(units):
            u = done('two')
            if done('one') < min(u + 2, len(units)):
                u = done('one')
                if units[u][0] // ROWS > sent:
                    break
                link = max(now, link) + wire * units[u][1] + pause
                got1[u] = link
                hops['one'].append(step)
            else:
                slack = 3 + SLACK * wire * (amount(u + 1) if u + 1 < len(units) else 0)
                if now < got1[u] + slack and u > must:
                    break
                now = max(now, got1[u])
                link = max(now, link) + wire * units[u][1] / 2 + pause
                core = max(now, core) + 2 * inner * units[u][1]
                got2[u] = max(link, core)
                hops['two'].append(step)
        while done('three') < done('two') and (got2[done('three')] + 3 <= now or done('three') <= must):
            u = done('three')
            now = max(now, got2[u])
            core = max(now, core) + inner * units[u][1]
            hops['three'].append(step)
        now += took[kind]
    for u in range(len(units)):
        hops['in'].append(first_use[u] - 1)
    return seq, units, hops


def layer(mesh, x_loc, cosine, sine, w_query, w_key, w_value, w_out):
    cp = mesh.shape['cp']
    rows, tok_rows, depth = x_loc.shape
    half_len = tok_rows // 2
    inner, kv_cols = w_query.shape[1], w_key.shape[1]
    heads = kv_cols // HEAD_DIM
    group_cols = inner // heads
    per_tile, fold = TILE // HEAD_DIM, TILE // HEAD_DIM // GROUP
    toks = ROWS * tok_rows
    chunks = rows // ROWS
    kt, qt, n_out = kv_cols // TILE, inner // TILE, depth // TILE
    n_proj = 2 * kt + qt
    per_chunk, total = ROWS * heads // STEP_HEADS, rows * heads // STEP_HEADS
    n_groups, per_group = heads // GROUP, GROUP // STEP_HEADS
    assert n_groups == 2
    assert depth == w_query.shape[0] and group_cols == 2 * PAIR and rows % ROWS == 0
    assert kt == 1 and n_proj > 4 and group_cols == GROUP * HEAD_DIM and cp // CORES == 4
    seq, units, hops = plan_steps(chunks, n_proj, n_out, per_chunk, 2 * kt)
    n_steps = len(seq)
    half_chunk, period = per_chunk // 2, per_chunk + n_out
    all_proj = n_proj * chunks
    first_a, second_a, last_a = (seq.index(('A', 0)), seq.index(('A', per_chunk)), seq.index(('S', total)))
    n_tiles = (n_proj + n_out) * chunks

    def pick(cases, other):
        for cond, val in reversed(cases):
            other = jnp.where(cond, val, other)
        return other

    def kern(x_hbm, cos_ref, sin_ref, wq_hbm, wk_hbm, wv_hbm, wo_hbm, y_hbm, kv_hbm, q_hbm,
             wbuf, xbuf, xres, raw, stage, oscr, ybuf, qbuf,
             wsem, xsem, rsem, osem, ysem, qsem, kvsem, send_sem, recv_sem, *attn):
        s = pl.program_id(0)
        my = lax.axis_index('cp')
        chip, core = div(my, CORES), rem(my, CORES)
        chips = cp // CORES

        def device(chip_shift, core_shift=0):
            return rem(chip + chip_shift, chips) * CORES + rem(core + core_shift, CORES)

        nxt, far, prv, mate = device(1), device(2), device(chips - 1), device(0, 1)

        a, r = 1 + div(s - second_a, period), rem(s - second_a, period)
        is_proj, is_flush = s < all_proj, s == all_proj
        in_first, is_skew = s < second_a, s == last_a
        past = jnp.where(s > last_a, period, 0)
        is_out = jnp.logical_or(past > 0, jnp.logical_and(jnp.logical_not(in_first), jnp.logical_and(r >= half_chunk, r < half_chunk + n_out)))
        is_head = jnp.logical_and(s > all_proj, jnp.logical_not(is_out))
        is_new = jnp.logical_and(is_head, jnp.logical_not(is_skew))
        n = jnp.where(in_first, s - first_a, a * per_chunk + jnp.where(r >= half_chunk + n_out, r - n_out, r))
        oidx = jnp.where(past > 0, s - last_a - 1 + (chunks - 1) * n_out, (a - 1) * n_out + r - half_chunk)
        pidx = s
        oc, col = div(oidx, n_out), rem(oidx, n_out)
        pc, pt = div(pidx, n_proj), rem(pidx, n_proj)
        tile_p, tile_o = pidx, all_proj + oidx

        def row_ds(c):
            return pl.ds(c * ROWS, ROWS)

        def load_tile(j):
            slot = rem(j, 2)
            is_p = j < all_proj
            p = rem(j, n_proj)
            o_chunk, o_col = div(j - all_proj, n_out), rem(j - all_proj, n_out)

            def start(w_hbm, tile_col):
                cols = pl.ds(pl.multiple_of(tile_col * TILE, TILE), TILE)
                part = w_hbm.shape[0] // SPLIT
                for i in range(SPLIT):
                    ks = pl.ds(i * part, part)
                    pltpu.make_async_copy(w_hbm.at[ks, cols], wbuf.at[slot, ks], wsem.at[slot]).start()

            @pl.when(jnp.logical_and(is_p, p < kt))
            def _():
                start(wk_hbm, p)

            @pl.when(jnp.logical_and(is_p, jnp.logical_and(p >= kt, p < 2 * kt)))
            def _():
                start(wv_hbm, p - kt)

            @pl.when(jnp.logical_and(is_p, p >= 2 * kt))
            def _():
                start(wq_hbm, p - 2 * kt)

            @pl.when(jnp.logical_not(is_p))
            def _():
                start(wo_hbm, o_col)
                load_res(o_chunk, o_col, slot).start()

        def load_res(c, tile_col, slot):
            cols = pl.ds(pl.multiple_of(tile_col * TILE, TILE), TILE)
            return pltpu.make_async_copy(x_hbm.at[row_ds(c), :, cols], xres.at[slot], rsem.at[slot])

        def next_tile(j):
            @pl.when(j + 1 < n_tiles)
            def _():
                load_tile(j + 1)
            slot = rem(j, 2)
            pltpu.make_async_copy(wo_hbm.at[:, pl.ds(0, TILE)], wbuf.at[slot], wsem.at[slot]).wait()
            return slot

        def load_x(c):
            return pltpu.make_async_copy(x_hbm.at[row_ds(c)], xbuf.at[rem(c, 2)], xsem.at[rem(c, 2)])

        def load_q(m):
            first = m * STEP_HEADS
            return pltpu.make_async_copy(q_hbm.at[div(first, heads), pl.ds(rem(first, heads), STEP_HEADS)], qbuf.at[rem(m, 2)], qsem.at[rem(m, 2)])

        def load_kv(g):
            slot = rem(g, 2)
            return [pltpu.make_async_copy(kv_hbm.at[div(g, n_groups), src, rem(g, n_groups)], attn[0].at[slot, src], kvsem.at[slot]) for src in range(cp)]

        def wait_kv(g):
            slot = rem(g, 2)
            pltpu.make_async_copy(kv_hbm.at[0, :, 0], attn[0].at[slot], kvsem.at[slot]).wait()

        def store_y(c, tile_col, slot):
            cols = pl.ds(pl.multiple_of(tile_col * TILE, TILE), TILE)
            return pltpu.make_async_copy(ybuf.at[slot], y_hbm.at[row_ds(c), :, cols], ysem.at[slot])

        def hop(kind, row, size, only=None, sem=0):
            rs = pl.ds(row, size)
            src, to = {R1: (my, nxt), L1: (my, prv), X0: (my, mate), R2: (prv, nxt), L2: (nxt, prv), X1: (nxt, mate), X2: (far, mate), X3: (prv, mate)}[kind]
            if kind in (R2, L2):
                ref = kv_hbm.at[rs, src, 0 if kind == R2 else 1]
            else:
                ref = kv_hbm.at[rs, src] if only is None else kv_hbm.at[rs, src, :, only]
            sem = 2 * row if only is None else sem
            return pltpu.make_async_remote_copy(src_ref=ref, dst_ref=ref, send_sem=send_sem.at[kind, sem], recv_sem=recv_sem.at[kind, sem],
                                                device_id={'cp': to}, device_id_type=pl.DeviceIdType.MESH)

        def first_copies(only, act):
            @pl.when(core == 0)
            def _():
                for kind in (R1, L1):
                    act(hop(kind, 0, ROWS, only, only))

            @pl.when(core != 0)
            def _():
                for kind in (R1, L1):
                    for i in range(ROWS):
                        act(hop(kind, i, 1, only, ROWS * only + i))

        def ring_one(row, size, act, parts=(0, 1)):
            @pl.when(row == 0)
            def _():
                for only in parts:
                    first_copies(only, act)

            @pl.when(row != 0)
            def _():
                near((R1, L1), row, size, act)

        def near(kinds, row, size, act):
            @pl.when(size == 1)
            def _():
                for kind in kinds:
                    act(hop(kind, row, 1))

            @pl.when(size != 1)
            def _():
                for kind in kinds:
                    act(hop(kind, row, ROWS))

        start, received, left = (lambda c: c.start()), (lambda c: c.wait_recv()), (lambda c: c.wait_send())

        def hop_one(row, size):
            ring_one(row, size, start, (1,))
            near((X0,), row, size, start)

        def hop_two(row, size):
            ring_one(row, size, received)
            near((R2, L2, X1, X3), row, size, start)

        def hop_three(row, size):
            near((R2, L2), row, size, received)
            near((X2,), row, size, start)

        def arrive(row, size):
            near((X0, X1, X3, X2), row, size, received)
            ring_one(row, size, left)
            near((R2, L2, X0, X1, X3, X2), row, size, left)
            for copy in load_kv(row * n_groups):
                copy.start()

            @pl.when(row == 0)
            def _():
                load_q(0).start()

        def unit_hops(lo, hi):
            for name, act in (('two', hop_two), ('one', hop_one), ('three', hop_three), ('in', arrive)):
                due = [(step, units[u]) for u, step in enumerate(hops[name]) if lo <= step < hi]
                if not due:
                    continue
                row, size = pick([(s == step, row) for step, (row, _) in due], -1), pick([(s == step, size) for step, (_, size) in due], ROWS)

                @pl.when(row >= 0)
                def _(row=row, size=size, act=act):
                    act(row, size)

        @pl.when(s == 0)
        def _():
            barrier = pltpu.get_barrier_semaphore()
            for to in (nxt, prv, mate):
                pl.semaphore_signal(barrier, inc=1, device_id={'cp': to}, device_id_type=pl.DeviceIdType.MESH)
            load_x(0).start()
            load_tile(0)
            attn_init(cp, attn)
            pl.semaphore_wait(barrier, 3)

        def store_tile(p):
            c, tile, slot = div(p, n_proj), rem(p, n_proj), rem(p, 2)
            rs = row_ds(c)

            @pl.when(tile < 2)
            def _():
                pltpu.make_async_copy(stage.at[slot], kv_hbm.at[rs, my, :, tile], osem.at[slot]).start()

            @pl.when(tile >= 2)
            def _():
                pltpu.make_async_copy(stage.at[slot], q_hbm.at[rs, pl.ds((tile - 2) * fold, fold)], osem.at[slot]).start()

        def wait_store(p):
            slot = rem(p, 2)
            pltpu.make_async_copy(stage.at[slot], q_hbm.at[pl.ds(0, ROWS), pl.ds(0, fold)], osem.at[slot]).wait()

        def rope_epilogue(p):
            c, slot = div(p, n_proj), rem(p, 2)
            is_v = rem(p, n_proj) == 1
            low_lanes = lax.broadcasted_iota(jnp.int32, (half_len, HEAD_DIM), 1) < HEAD_DIM // 2
            for i in range(ROWS):
                ts = pl.ds(pl.multiple_of((c * ROWS + i) * half_len, half_len), half_len)
                cos, sin = cos_ref[ts], sin_ref[ts]
                cos_r, sin_r = pltpu.roll(cos, HEAD_DIM // 2, 1), pltpu.roll(sin, HEAD_DIM // 2, 1)
                for half in range(2):
                    cos_h = jnp.where(low_lanes, cos, cos_r) if half == 0 else jnp.where(low_lanes, cos_r, cos)
                    sin_h = jnp.where(low_lanes, -sin, sin_r) if half == 0 else jnp.where(low_lanes, -sin_r, sin)
                    rs = slice(i * tok_rows + half * half_len, i * tok_rows + (half + 1) * half_len)
                    for e in range(per_tile):
                        vals = raw[rs, e * HEAD_DIM:(e + 1) * HEAD_DIM]
                        wide = vals.astype(f32)
                        turned = (wide * cos_h + pltpu.roll(wide, HEAD_DIM // 2, 1) * sin_h).astype(bf16)
                        stage[slot, i, e // GROUP, half, e % GROUP] = jnp.where(is_v, vals.T, turned)

        @pl.when(is_proj)
        def _():
            next_tile(tile_p)

            @pl.when(jnp.logical_and(pidx > 3, pt != 4))
            def _():
                wait_store(pidx - 3)

            @pl.when(pidx == 2)
            def _():
                wait_store(0)
                first_copies(0, start)

            @pl.when(pt == 3)
            def _():
                wait_store(pidx - 2)

            @pl.when(pt == 0)
            def _():
                load_x(pc).wait()

            @pl.when(jnp.logical_and(pt == 1, pc + 1 < chunks))
            def _():
                load_x(pc + 1).start()

        spans = 6
        for i in range(spans):
            lo, hi = n_steps * i // spans, n_steps * (i + 1) // spans

            @pl.when(jnp.logical_and(s >= lo, s < hi))
            def _(lo=lo, hi=hi):
                unit_hops(lo, hi)

        @pl.when(is_proj)
        def _():
            rope_epilogue(jnp.maximum(pidx - 1, 0))
            x = xbuf[rem(pc, 2)].reshape(toks, depth)
            raw[...] = jnp.dot(x, wbuf[rem(tile_p, 2)], preferred_element_type=f32).astype(bf16)

            @pl.when(pidx >= 1)
            def _():
                store_tile(pidx - 1)

        @pl.when(is_flush)
        def _():
            end = n_proj * chunks
            wait_store(end - 3)
            rope_epilogue(end - 1)
            store_tile(end - 1)
            wait_store(end - 2)
            wait_store(end - 1)

        def attend(head, slot, i):
            m = jnp.maximum(head - 1, 0)
            o_slot = rem(div(m, ROWS * heads), 2)
            row, h = rem(div(m, heads), ROWS), rem(m, heads)

            def put(half, j, val):
                rs = pl.ds(pl.multiple_of(row * tok_rows + half * half_len, half_len), half_len)
                cs = pl.ds(pl.multiple_of(h * group_cols + j * HEAD_DIM, HEAD_DIM), HEAD_DIM)
                oscr[o_slot, rs, cs] = val

            attn_step(head, cp, my, qbuf.at[slot, i], put, attn)

        @pl.when(is_new)
        def _():
            g = div(n, per_group)
            load_q(n).wait()

            @pl.when(n + 1 < total)
            def _():
                load_q(n + 1).start()

            @pl.when(rem(n, per_group) == 0)
            def _():
                wait_kv(g)

            fresh = jnp.logical_or(rem(g + 1, ROWS * n_groups) == 0, jnp.logical_and(g + 1 >= (rows - SINGLE * ROWS) * n_groups, rem(g + 1, n_groups) == 0))

            @pl.when(jnp.logical_and(rem(n, per_group) == per_group - 1, jnp.logical_not(fresh)))
            def _():
                for copy in load_kv(g + 1):
                    copy.start()

            for i in range(STEP_HEADS):
                attend(n * STEP_HEADS + i, rem(n, 2), i)

        @pl.when(is_skew)
        def _():
            attend(n * STEP_HEADS, rem(n, 2), 0)

        @pl.when(is_out)
        def _():
            slot = next_tile(tile_o)
            y_slot = rem(oidx, 2)
            load_res(oc, col, slot).wait()

            @pl.when(oidx >= 2)
            def _():
                store_y(0, 0, y_slot).wait()

            out = jnp.dot(oscr[rem(oc, 2)], wbuf[slot], preferred_element_type=f32)
            ybuf[y_slot] = (xres[slot].astype(f32) + out.reshape(ROWS, tok_rows, TILE)).astype(bf16)
            store_y(oc, col, y_slot).start()

            @pl.when(oidx == n_out * chunks - 1)
            def _():
                store_y(0, 0, 1 - y_slot).wait()
                store_y(0, 0, y_slot).wait()

    any_spec = pl.BlockSpec(memory_space=pl.ANY)
    flops = 2 * rows * tok_rows * depth * (2 * inner + 2 * kv_cols) + 8 * rows * heads * (cp + 1) * half_len * group_cols * HEAD_DIM * 2
    y, _, _ = pl.pallas_call(
        kern,
        name='layer',
        grid=(n_steps,),
        in_specs=[any_spec, pl.BlockSpec(memory_space=pltpu.VMEM), pl.BlockSpec(memory_space=pltpu.VMEM)] + [any_spec] * 4,
        out_specs=[any_spec] * 3,
        out_shape=[
            jax.ShapeDtypeStruct(x_loc.shape, bf16),
            jax.ShapeDtypeStruct((rows, cp, n_groups, 2, 2, GROUP, half_len, HEAD_DIM), bf16),
            jax.ShapeDtypeStruct((rows, heads, 2, group_cols // HEAD_DIM, half_len, HEAD_DIM), bf16),
        ],
        scratch_shapes=[
            pltpu.VMEM((2, depth, TILE), bf16),
            pltpu.VMEM((2, ROWS, tok_rows, depth), bf16),
            pltpu.VMEM((2, ROWS, tok_rows, TILE), bf16),
            pltpu.VMEM((toks, TILE), bf16),
            pltpu.VMEM((2, ROWS, fold, 2, GROUP, half_len, HEAD_DIM), bf16),
            pltpu.VMEM((2, toks, inner), bf16),
            pltpu.VMEM((2, ROWS, tok_rows, TILE), bf16),
            pltpu.VMEM((2, STEP_HEADS, 2, group_cols // HEAD_DIM, half_len, HEAD_DIM), bf16),
            pltpu.SemaphoreType.DMA((2,)),
            pltpu.SemaphoreType.DMA((2,)),
            pltpu.SemaphoreType.DMA((2,)),
            pltpu.SemaphoreType.DMA((2,)),
            pltpu.SemaphoreType.DMA((2,)),
            pltpu.SemaphoreType.DMA((2,)),
            pltpu.SemaphoreType.DMA((2,)),
            pltpu.SemaphoreType.DMA((8, 2 * rows)),
            pltpu.SemaphoreType.DMA((8, 2 * rows)),
        ] + attn_scratch(cp, half_len),
        compiler_params=pltpu.CompilerParams(dimension_semantics=('arbitrary',), collective_id=0, has_side_effects=True, vmem_limit_bytes=VMEM_LIMIT),
        cost_estimate=pl.CostEstimate(flops=flops, bytes_accessed=4 * rows * tok_rows * depth, transcendentals=0),
    )(x_loc, cosine, sine, w_query, w_key, w_value, w_out)
    return y


def solution(mesh):
    row_spec, pos_spec, rep_spec = P('data', 'cp', None), P('data', 'cp'), P(None, None)

    def local_block(x_loc, pos_loc, w_query, w_key, w_value, w_out):
        cosine, sine = rope_tables(pos_loc)
        return layer(mesh, x_loc, cosine, sine, w_query, w_key, w_value, w_out)

    return jax.shard_map(local_block, mesh=mesh, in_specs=(row_spec, pos_spec, rep_spec, rep_spec, rep_spec, rep_spec), out_specs=row_spec, check_vma=False)
```

```python
import functools
import math

import jax
import jax.numpy as jnp
from jax import lax
from jax.experimental import pallas as pl
from jax.experimental.pallas import tpu as pltpu
from jax.sharding import PartitionSpec as P

HEAD_DIM = 128
ROPE_BASE = 500000
MASK_FILL = -1e30
EXP_SCALE = float(HEAD_DIM ** -0.5 * math.log2(math.e))
CORES = 2
ROWS = 2
TILE = 1024
GROUP = 4
STEP_HEADS = 4
PAIR = 256
VMEM_LIMIT = 66_000_000
LAG = 5
DELAY = 2
BACK = (2, 0)
EPI = 3
SINGLE = 2
COST = (4.85, 4.72, 4.9, 22.8, 0.4, 1.75, 18.0)
SLACK = 0.3
SPLIT = 4
R1, L1, X0, R2, L2, X1, X2, X3 = range(8)
f32, bf16 = jnp.float32, jnp.bfloat16
div, rem = lax.div, lax.rem


def rope_tables(positions):
    half = HEAD_DIM // 2
    inv_freq = 1.0 / (ROPE_BASE ** (jnp.arange(0, HEAD_DIM, 2, dtype=f32) / HEAD_DIM))
    half_len = positions.shape[1] // 2
    pos = positions.astype(f32)
    front = jnp.broadcast_to(pos[:, :half_len, None], pos[:, :half_len].shape + (half,))
    back = jnp.broadcast_to(pos[:, half_len:, None], front.shape)
    angles = (jnp.concatenate([front, back], axis=-1) * jnp.concatenate([inv_freq, inv_freq])).reshape(-1, HEAD_DIM)
    return jnp.cos(angles), jnp.sin(angles)


def attn_steps(cp):
    dyn = cp // 2 - 1
    return ['front'] + ['extra'] + [('pair', k) for k in range(dyn)] + ['back'] + [('pair', k) for k in range(dyn, cp - 1)]


def attn_scratch(cp, half_len):
    steps = attn_steps(cp)
    blocks = sum(1 if isinstance(t, str) else 2 for t in steps)
    groups = lambda *shape: [pltpu.VMEM(shape, f32), pltpu.VMEM(shape, f32)]
    return [
        pltpu.VMEM((2, cp, 2, GROUP, half_len, HEAD_DIM), bf16),
        pltpu.VMEM((3, cp, 2, GROUP, HEAD_DIM, half_len), bf16),
        *groups(blocks * half_len, PAIR),
        *groups(1 + len(BACK), HEAD_DIM, PAIR),
        *groups(cp // 2 + 1, HEAD_DIM, PAIR),
        *groups(2, 1, PAIR),
        *groups(2, 1, PAIR),
        pltpu.VMEM((half_len, half_len), f32),
    ]


def attn_init(cp, scratch):
    _, _, _, _, _, _, pv0, pv1, _, _, _, _, bias = scratch
    kpos = lax.broadcasted_iota(jnp.int32, bias.shape, 0)
    qpos = lax.broadcasted_iota(jnp.int32, bias.shape, 1)
    for ref in (pv0, pv1):
        ref[ref.shape[0] - 1] = jnp.zeros(ref.shape[1:], f32)
    bias[...] = jnp.where(kpos <= qpos, 0.0, MASK_FILL)


def attn_step(n, cp, my, q_ref, put, scratch):
    kbuf, vbuf, sc0, sc1, ac0, ac1, pv0, pv1, mx0, mx1, sm0, sm1, bias = scratch
    sbuf, acc, pvb, mst, lst = (sc0, sc1), (ac0, ac1), (pv0, pv1), (mx0, mx1), (sm0, sm1)
    steps, parts = attn_steps(cp), cp // 2
    half_len = kbuf.shape[4]
    here, k_slot = (rem(div(n, GROUP), 3), rem(n, GROUP)), rem(div(n, GROUP), 2)
    before = jnp.maximum(n - 1, 0)
    behind_ = (rem(div(before, GROUP), 3), rem(before, GROUP))
    pairs, par = div(my, 2), rem(my, 2)

    def place(j):
        front = j < cp
        return jnp.where(front, j, 2 * cp - 1 - j), jnp.where(front, 0, 1)

    front_of, part_of, locs, rows_of, row = {}, {}, {}, {}, 0
    for t in steps:
        if t == 'front':
            front_of[t], blocks = True, [my]
        elif t == 'back':
            front_of[t], blocks = False, [2 * cp - 1 - my]
        elif t == 'extra':
            front_of[t], part_of[t], blocks = par == 1, 0, [jnp.where(par == 1, my - 1, 2 * cp - 2 - my)]
        else:
            k = t[1]
            if k < parts - 1:
                front_of[t], part_of[t] = k < pairs, 1 + k
                first = 2 * jnp.where(k < pairs, k, k - pairs)
            else:
                front_of[t], first = False, 2 * (k - pairs)
            blocks = [first, first + 1]
        locs[t] = [place(j) for j in blocks]
        rows_of[t] = slice(row, row + len(blocks) * half_len)
        row += len(blocks) * half_len
    low = jnp.full((1, PAIR), MASK_FILL, f32)
    zero = jnp.zeros((1, PAIR), f32)

    def half_of(t):
        return jnp.where(front_of[t], 0, 1) if t in part_of else 0 if front_of[t] else 1

    def stack(items, axis):
        return items[0] if len(items) == 1 else jnp.concatenate(items, axis=axis)

    def scores(t, g):
        e = here[1]
        k = stack([kbuf[k_slot, s, f, e] for s, f in locs[t]], 0)
        s = lax.dot_general(k, q_ref[half_of(t), 2 * g:2 * g + 2].reshape(PAIR, HEAD_DIM), (((1,), (1,)), ((), ())), preferred_element_type=f32)
        if t in ('front', 'back'):
            b = bias[...]
            s = s + jnp.concatenate([b, b], axis=1)
        sbuf[g][rows_of[t]] = s
        return jnp.max(s, axis=0, keepdims=True)

    def finish_max(g, ms):
        front_max, back_max = low, low
        for t, m in zip(steps, ms):
            if t in part_of:
                front_max = jnp.maximum(front_max, jnp.where(front_of[t], m, low))
                back_max = jnp.maximum(back_max, jnp.where(front_of[t], low, m))
            elif front_of[t]:
                front_max = jnp.maximum(front_max, m)
            else:
                back_max = jnp.maximum(back_max, m)
        mst[g][0] = front_max
        mst[g][1] = back_max

    def soft(t, g, behind):
        m = mst[g][half_of(t)]
        if behind is not None:
            m = jnp.maximum(m, jnp.minimum(behind, MASK_FILL))
        p = jnp.exp2((sbuf[g][rows_of[t]] - m) * EXP_SCALE)
        return jnp.sum(p, axis=0, keepdims=True), p.astype(bf16)

    def put_weighted(g, ts, ps, at):
        slot, e = at
        vals = stack([vbuf[slot, s, f, e] for t in ts for s, f in locs[t]], 1)
        out = lax.dot_general(vals, stack(ps, 0), (((1,), (0,)), ((), ())), preferred_element_type=f32)
        if ts[0] in part_of:
            pvb[g][part_of[ts[0]]] = out
        elif front_of[ts[0]]:
            acc[g][0] = out
        else:
            acc[g][1 + BACK.index(len(steps) - 1 - steps.index(ts[-1]))] = out

    def epilogue(g):
        for half in range(2):
            inv = 1.0 / lst[g][half]
            for e in range(PAIR // HEAD_DIM):
                lanes = slice(e * half_len, (e + 1) * half_len)
                o = acc[g][half, :, lanes]
                for i in range(1, len(BACK) if half else 1):
                    o = o + acc[g][1 + i, :, lanes]
                for t, part in part_of.items():
                    mine = front_of[t] if half == 0 else jnp.logical_not(front_of[t])
                    o = o + pvb[g][jnp.where(mine, part, parts), :, lanes]
                put(half, g * (PAIR // HEAD_DIM) + e, (o * inv[:, lanes]).astype(bf16).T)
                yield

    pending = []

    def drain(limit):
        while len(pending) > limit:
            put_weighted(*pending.pop(0))

    for g1, g2, at in ((0, 1, behind_), (1, 0, here)):
        epi = epilogue(g1)
        ms, front_sum, back_sum, held = [], zero, zero, []
        for i, t in enumerate(steps):
            ms.append(scores(t, g1))
            l, p = soft(t, g2, ms[i - LAG] if i >= LAG else None)
            if t in part_of:
                front_sum = front_sum + jnp.where(front_of[t], l, zero)
                back_sum = back_sum + jnp.where(front_of[t], zero, l)
            elif front_of[t]:
                front_sum = front_sum + l
            else:
                back_sum = back_sum + l
            if t in part_of or front_of[t]:
                pending.append((g2, [t], [p], at))
            else:
                held.append((t, p))
                if len(steps) - 1 - i in BACK:
                    pending.append((g2, [t for t, _ in held], [p for _, p in held], at))
                    held = []
            drain(DELAY)
            if i >= EPI:
                next(epi, None)
        lst[g2][0] = front_sum
        lst[g2][1] = back_sum
        finish_max(g1, ms)
        for _ in epi:
            pass
    drain(0)


def plan_steps(chunks, n_proj, n_out, per_chunk, send_at):
    half = per_chunk // 2
    seq = [('P', i) for i in range(chunks * n_proj)] + [('F', 0)]
    for c in range(chunks):
        seq += [('A', c * per_chunk + i) for i in range(half)]
        if c:
            seq += [('O', (c - 1) * n_out + i) for i in range(n_out)]
        seq += [('A', c * per_chunk + i) for i in range(half, per_chunk)]
    seq += [('S', chunks * per_chunk)] + [('O', (chunks - 1) * n_out + i) for i in range(n_out)]
    units = [(c * ROWS, ROWS) for c in range(chunks - SINGLE)] + [(i, 1) for i in range((chunks - SINGLE) * ROWS, chunks * ROWS)]
    first_use = [seq.index(('A', row * per_chunk // ROWS)) for row, _ in units]
    proj, out, att, wire, pause, inner, now = COST
    took = {'P': proj, 'O': out, 'A': att, 'S': att, 'F': 0.6}
    amount = lambda u: units[u][1]
    hops = {'one': [], 'two': [], 'three': [], 'in': []}
    link, core, got1, got2, sent = 0.0, 0.0, {}, {}, -1
    for step, (kind, i) in enumerate(seq):
        if step and seq[step - 1][0] == 'P' and seq[step - 1][1] % n_proj == send_at:
            sent = seq[step - 1][1] // n_proj
        must = max((u for u in range(len(units)) if first_use[u] <= step + 1), default=-1)
        done = lambda name: len(hops[name])
        while done('one') < len(units) or done('two') < len(units):
            u = done('two')
            if done('one') < min(u + 2, len(units)):
                u = done('one')
                if units[u][0] // ROWS > sent:
                    break
                link = max(now, link) + wire * units[u][1] + pause
                got1[u] = link
                hops['one'].append(step)
            else:
                slack = 3 + SLACK * wire * (amount(u + 1) if u + 1 < len(units) else 0)
                if now < got1[u] + slack and u > must:
                    break
                now = max(now, got1[u])
                link = max(now, link) + wire * units[u][1] / 2 + pause
                core = max(now, core) + 2 * inner * units[u][1]
                got2[u] = max(link, core)
                hops['two'].append(step)
        while done('three') < done('two') and (got2[done('three')] + 3 <= now or done('three') <= must):
            u = done('three')
            now = max(now, got2[u])
            core = max(now, core) + inner * units[u][1]
            hops['three'].append(step)
        now += took[kind]
    for u in range(len(units)):
        hops['in'].append(first_use[u] - 1)
    return seq, units, hops


def layer(mesh, x_loc, cosine, sine, w_query, w_key, w_value, w_out):
    cp = mesh.shape['cp']
    rows, tok_rows, depth = x_loc.shape
    half_len = tok_rows // 2
    inner, kv_cols = w_query.shape[1], w_key.shape[1]
    heads = kv_cols // HEAD_DIM
    group_cols = inner // heads
    per_tile, fold = TILE // HEAD_DIM, TILE // HEAD_DIM // GROUP
    toks = ROWS * tok_rows
    chunks = rows // ROWS
    kt, qt, n_out = kv_cols // TILE, inner // TILE, depth // TILE
    n_proj = 2 * kt + qt
    per_chunk, total = ROWS * heads // STEP_HEADS, rows * heads // STEP_HEADS
    n_groups, per_group = heads // GROUP, GROUP // STEP_HEADS
    assert n_groups == 2
    assert depth == w_query.shape[0] and group_cols == 2 * PAIR and rows % ROWS == 0
    assert kt == 1 and n_proj > 4 and group_cols == GROUP * HEAD_DIM and cp // CORES == 4
    seq, units, hops = plan_steps(chunks, n_proj, n_out, per_chunk, 2 * kt)
    n_steps = len(seq)
    half_chunk, period = per_chunk // 2, per_chunk + n_out
    all_proj = n_proj * chunks
    first_a, second_a, last_a = (seq.index(('A', 0)), seq.index(('A', per_chunk)), seq.index(('S', total)))
    n_tiles = (n_proj + n_out) * chunks

    def pick(cases, other):
        for cond, val in reversed(cases):
            other = jnp.where(cond, val, other)
        return other

    def kern(x_hbm, cos_hbm, sin_hbm, wq_hbm, wk_hbm, wv_hbm, wo_hbm, y_hbm, kv_hbm, q_hbm,
             wbuf, xbuf, tables, xres, raw, stage, oscr, ybuf, qbuf,
             wsem, xsem, tsem, rsem, osem, ysem, qsem, ksem, vsem, send_sem, recv_sem, *attn):
        s = pl.program_id(0)
        my = lax.axis_index('cp')
        chip, core = div(my, CORES), rem(my, CORES)
        chips = cp // CORES

        def device(chip_shift, core_shift=0):
            return rem(chip + chip_shift, chips) * CORES + rem(core + core_shift, CORES)

        nxt, far, prv, mate = device(1), device(2), device(chips - 1), device(0, 1)

        a, r = 1 + div(s - second_a, period), rem(s - second_a, period)
        is_proj, is_flush = s < all_proj, s == all_proj
        in_first, is_skew = s < second_a, s == last_a
        past = jnp.where(s > last_a, period, 0)
        is_out = jnp.logical_or(past > 0, jnp.logical_and(jnp.logical_not(in_first), jnp.logical_and(r >= half_chunk, r < half_chunk + n_out)))
        is_head = jnp.logical_and(s > all_proj, jnp.logical_not(is_out))
        is_new = jnp.logical_and(is_head, jnp.logical_not(is_skew))
        n = jnp.where(in_first, s - first_a, a * per_chunk + jnp.where(r >= half_chunk + n_out, r - n_out, r))
        oidx = jnp.where(past > 0, s - last_a - 1 + (chunks - 1) * n_out, (a - 1) * n_out + r - half_chunk)
        pidx = s
        oc, col = div(oidx, n_out), rem(oidx, n_out)
        pc, pt = div(pidx, n_proj), rem(pidx, n_proj)
        tile_p, tile_o = pidx, all_proj + oidx

        def row_ds(c):
            return pl.ds(c * ROWS, ROWS)

        def load_tile(j):
            slot = rem(j, 2)
            is_p = j < all_proj
            p = rem(j, n_proj)
            o_chunk, o_col = div(j - all_proj, n_out), rem(j - all_proj, n_out)

            def start(w_hbm, tile_col):
                cols = pl.ds(pl.multiple_of(tile_col * TILE, TILE), TILE)
                part = w_hbm.shape[0] // SPLIT
                for i in range(SPLIT):
                    ks = pl.ds(i * part, part)
                    pltpu.make_async_copy(w_hbm.at[ks, cols], wbuf.at[slot, ks], wsem.at[slot]).start()

            @pl.when(jnp.logical_and(is_p, p < kt))
            def _():
                start(wk_hbm, p)

            @pl.when(jnp.logical_and(is_p, jnp.logical_and(p >= kt, p < 2 * kt)))
            def _():
                start(wv_hbm, p - kt)

            @pl.when(jnp.logical_and(is_p, p >= 2 * kt))
            def _():
                start(wq_hbm, p - 2 * kt)

            @pl.when(jnp.logical_not(is_p))
            def _():
                start(wo_hbm, o_col)
                load_res(o_chunk, o_col, slot).start()

        def load_res(c, tile_col, slot):
            cols = pl.ds(pl.multiple_of(tile_col * TILE, TILE), TILE)
            return pltpu.make_async_copy(x_hbm.at[row_ds(c), :, cols], xres.at[slot], rsem.at[slot])

        def next_tile(j):
            @pl.when(j + 1 < n_tiles)
            def _():
                load_tile(j + 1)
            slot = rem(j, 2)
            pltpu.make_async_copy(wo_hbm.at[:, pl.ds(0, TILE)], wbuf.at[slot], wsem.at[slot]).wait()
            return slot

        def load_x(c):
            return pltpu.make_async_copy(x_hbm.at[row_ds(c)], xbuf.at[rem(c, 2)], xsem.at[rem(c, 2)])

        def load_tables(c):
            ts, slot = pl.ds(pl.multiple_of(c * ROWS * half_len, ROWS * half_len), ROWS * half_len), rem(c, 2)
            return [pltpu.make_async_copy(src.at[ts], tables.at[slot, i], tsem.at[slot]) for i, src in enumerate((cos_hbm, sin_hbm))]

        def load_q(m):
            first = m * STEP_HEADS
            return pltpu.make_async_copy(q_hbm.at[div(first, heads), pl.ds(rem(first, heads), STEP_HEADS)], qbuf.at[rem(m, 2)], qsem.at[rem(m, 2)])

        def load_kv(g):
            row, group, slots = div(g, n_groups), rem(g, n_groups), (rem(g, 2), rem(g, 3))
            return [pltpu.make_async_copy(kv_hbm.at[row, src, group, i], attn[i].at[slots[i], src], sem.at[slots[i]])
                    for i, sem in enumerate((ksem, vsem)) for src in range(cp)]

        def wait_kv(g):
            for i, (sem, slot) in enumerate(((ksem, rem(g, 2)), (vsem, rem(g, 3)))):
                pltpu.make_async_copy(kv_hbm.at[0, :, 0, i], attn[i].at[slot], sem.at[slot]).wait()

        def store_y(c, tile_col, slot):
            cols = pl.ds(pl.multiple_of(tile_col * TILE, TILE), TILE)
            return pltpu.make_async_copy(ybuf.at[slot], y_hbm.at[row_ds(c), :, cols], ysem.at[slot])

        def hop(kind, row, size, only=None, sem=0):
            rs = pl.ds(row, size)
            src, to = {R1: (my, nxt), L1: (my, prv), X0: (my, mate), R2: (prv, nxt), L2: (nxt, prv), X1: (nxt, mate), X2: (far, mate), X3: (prv, mate)}[kind]
            if kind in (R2, L2):
                ref = kv_hbm.at[rs, src, 0 if kind == R2 else 1]
            else:
                ref = kv_hbm.at[rs, src] if only is None else kv_hbm.at[rs, src, :, only]
            sem = 2 * row if only is None else sem
            return pltpu.make_async_remote_copy(src_ref=ref, dst_ref=ref, send_sem=send_sem.at[kind, sem], recv_sem=recv_sem.at[kind, sem],
                                                device_id={'cp': to}, device_id_type=pl.DeviceIdType.MESH)

        def first_copies(only, act):
            @pl.when(core == 0)
            def _():
                for kind in (R1, L1):
                    act(hop(kind, 0, ROWS, only, only))

            @pl.when(core != 0)
            def _():
                for kind in (R1, L1):
                    for i in range(ROWS):
                        act(hop(kind, i, 1, only, ROWS * only + i))

        def ring_one(row, size, act, parts=(0, 1)):
            @pl.when(row == 0)
            def _():
                for only in parts:
                    first_copies(only, act)

            @pl.when(row != 0)
            def _():
                near((R1, L1), row, size, act)

        def near(kinds, row, size, act):
            @pl.when(size == 1)
            def _():
                for kind in kinds:
                    act(hop(kind, row, 1))

            @pl.when(size != 1)
            def _():
                for kind in kinds:
                    act(hop(kind, row, ROWS))

        start, received, left = (lambda c: c.start()), (lambda c: c.wait_recv()), (lambda c: c.wait_send())

        def hop_one(row, size):
            ring_one(row, size, start, (1,))
            near((X0,), row, size, start)

        def hop_two(row, size):
            ring_one(row, size, received)
            near((R2, L2, X1, X3), row, size, start)

        def hop_three(row, size):
            near((R2, L2), row, size, received)
            near((X2,), row, size, start)

        def arrive(row, size):
            near((X0, X1, X3, X2), row, size, received)
            ring_one(row, size, left)
            near((R2, L2, X0, X1, X3, X2), row, size, left)
            for copy in load_kv(row * n_groups):
                copy.start()

            @pl.when(row == 0)
            def _():
                load_q(0).start()

        def unit_hops(lo, hi):
            for name, act in (('two', hop_two), ('one', hop_one), ('three', hop_three), ('in', arrive)):
                due = [(step, units[u]) for u, step in enumerate(hops[name]) if lo <= step < hi]
                if not due:
                    continue
                row, size = pick([(s == step, row) for step, (row, _) in due], -1), pick([(s == step, size) for step, (_, size) in due], ROWS)

                @pl.when(row >= 0)
                def _(row=row, size=size, act=act):
                    act(row, size)

        @pl.when(s == 0)
        def _():
            barrier = pltpu.get_barrier_semaphore()
            for to in (nxt, prv, mate):
                pl.semaphore_signal(barrier, inc=1, device_id={'cp': to}, device_id_type=pl.DeviceIdType.MESH)
            load_x(0).start()
            for copy in load_tables(0):
                copy.start()
            load_tile(0)
            attn_init(cp, attn)
            pl.semaphore_wait(barrier, 3)

        def store_tile(p):
            c, tile, slot = div(p, n_proj), rem(p, n_proj), rem(p, 2)
            rs = row_ds(c)

            @pl.when(tile < 2)
            def _():
                pltpu.make_async_copy(stage.at[slot], kv_hbm.at[rs, my, :, tile], osem.at[slot]).start()

            @pl.when(tile >= 2)
            def _():
                pltpu.make_async_copy(stage.at[slot], q_hbm.at[rs, pl.ds((tile - 2) * fold, fold)], osem.at[slot]).start()

        def wait_store(p):
            slot = rem(p, 2)
            pltpu.make_async_copy(stage.at[slot], q_hbm.at[pl.ds(0, ROWS), pl.ds(0, fold)], osem.at[slot]).wait()

        def rope_epilogue(p):
            c, slot = div(p, n_proj), rem(p, 2)
            is_v = rem(p, n_proj) == 1
            low_lanes = lax.broadcasted_iota(jnp.int32, (half_len, HEAD_DIM), 1) < HEAD_DIM // 2
            for i in range(ROWS):
                ts = slice(i * half_len, (i + 1) * half_len)
                cos, sin = tables[rem(c, 2), 0, ts], tables[rem(c, 2), 1, ts]
                cos_r, sin_r = pltpu.roll(cos, HEAD_DIM // 2, 1), pltpu.roll(sin, HEAD_DIM // 2, 1)
                for half in range(2):
                    cos_h = jnp.where(low_lanes, cos, cos_r) if half == 0 else jnp.where(low_lanes, cos_r, cos)
                    sin_h = jnp.where(low_lanes, -sin, sin_r) if half == 0 else jnp.where(low_lanes, -sin_r, sin)
                    rs = slice(i * tok_rows + half * half_len, i * tok_rows + (half + 1) * half_len)
                    for e in range(per_tile):
                        vals = raw[rs, e * HEAD_DIM:(e + 1) * HEAD_DIM]
                        wide = vals.astype(f32)
                        turned = (wide * cos_h + pltpu.roll(wide, HEAD_DIM // 2, 1) * sin_h).astype(bf16)
                        stage[slot, i, e // GROUP, half, e % GROUP] = jnp.where(is_v, vals.T, turned)

        @pl.when(is_proj)
        def _():
            next_tile(tile_p)

            @pl.when(jnp.logical_and(pidx > 3, pt != 4))
            def _():
                wait_store(pidx - 3)

            @pl.when(pidx == 2)
            def _():
                wait_store(0)
                first_copies(0, start)

            @pl.when(pt == 3)
            def _():
                wait_store(pidx - 2)

            @pl.when(pt == 0)
            def _():
                load_x(pc).wait()

            @pl.when(jnp.where(pc == 0, pt == 0, pt == 1))
            def _():
                for copy in load_tables(pc):
                    copy.wait()

            @pl.when(pt == 1)
            def _():
                @pl.when(pc + 1 < chunks)
                def _():
                    load_x(pc + 1).start()
                    for copy in load_tables(pc + 1):
                        copy.start()

        spans = 6
        for i in range(spans):
            lo, hi = n_steps * i // spans, n_steps * (i + 1) // spans

            @pl.when(jnp.logical_and(s >= lo, s < hi))
            def _(lo=lo, hi=hi):
                unit_hops(lo, hi)

        @pl.when(is_proj)
        def _():
            rope_epilogue(jnp.maximum(pidx - 1, 0))
            x = xbuf[rem(pc, 2)].reshape(toks, depth)
            raw[...] = jnp.dot(x, wbuf[rem(tile_p, 2)], preferred_element_type=f32).astype(bf16)

            @pl.when(pidx >= 1)
            def _():
                store_tile(pidx - 1)

        @pl.when(is_flush)
        def _():
            end = n_proj * chunks
            wait_store(end - 3)
            rope_epilogue(end - 1)
            store_tile(end - 1)
            wait_store(end - 2)
            wait_store(end - 1)

        def attend(head, slot, i):
            m = jnp.maximum(head - 1, 0)
            o_slot = rem(div(m, ROWS * heads), 2)
            row, h = rem(div(m, heads), ROWS), rem(m, heads)

            def put(half, j, val):
                rs = pl.ds(pl.multiple_of(row * tok_rows + half * half_len, half_len), half_len)
                cs = pl.ds(pl.multiple_of(h * group_cols + j * HEAD_DIM, HEAD_DIM), HEAD_DIM)
                oscr[o_slot, rs, cs] = val

            attn_step(head, cp, my, qbuf.at[slot, i], put, attn)

        @pl.when(is_new)
        def _():
            g = div(n, per_group)
            load_q(n).wait()

            @pl.when(n + 1 < total)
            def _():
                load_q(n + 1).start()

            @pl.when(rem(n, per_group) == 0)
            def _():
                wait_kv(g)

            fresh = jnp.logical_or(rem(g + 1, ROWS * n_groups) == 0, jnp.logical_and(g + 1 >= (rows - SINGLE * ROWS) * n_groups, rem(g + 1, n_groups) == 0))

            @pl.when(jnp.logical_and(rem(n, per_group) == 0, jnp.logical_not(fresh)))
            def _():
                for copy in load_kv(g + 1):
                    copy.start()

            for i in range(STEP_HEADS):
                attend(n * STEP_HEADS + i, rem(n, 2), i)

        @pl.when(is_skew)
        def _():
            attend(n * STEP_HEADS, rem(n, 2), 0)

        @pl.when(is_out)
        def _():
            slot = next_tile(tile_o)
            y_slot = rem(oidx, 2)
            load_res(oc, col, slot).wait()

            @pl.when(oidx >= 2)
            def _():
                store_y(0, 0, y_slot).wait()

            out = jnp.dot(oscr[rem(oc, 2)], wbuf[slot], preferred_element_type=f32)
            ybuf[y_slot] = (xres[slot].astype(f32) + out.reshape(ROWS, tok_rows, TILE)).astype(bf16)
            store_y(oc, col, y_slot).start()

            @pl.when(oidx == n_out * chunks - 1)
            def _():
                store_y(0, 0, 1 - y_slot).wait()
                store_y(0, 0, y_slot).wait()

    any_spec = pl.BlockSpec(memory_space=pl.ANY)
    flops = 2 * rows * tok_rows * depth * (2 * inner + 2 * kv_cols) + 8 * rows * heads * (cp + 1) * half_len * group_cols * HEAD_DIM * 2
    y, _, _ = pl.pallas_call(
        kern,
        name='layer',
        grid=(n_steps,),
        in_specs=[any_spec] * 7,
        out_specs=[any_spec] * 3,
        out_shape=[
            jax.ShapeDtypeStruct(x_loc.shape, bf16),
            jax.ShapeDtypeStruct((rows, cp, n_groups, 2, 2, GROUP, half_len, HEAD_DIM), bf16),
            jax.ShapeDtypeStruct((rows, heads, 2, group_cols // HEAD_DIM, half_len, HEAD_DIM), bf16),
        ],
        scratch_shapes=[
            pltpu.VMEM((2, depth, TILE), bf16),
            pltpu.VMEM((2, ROWS, tok_rows, depth), bf16),
            pltpu.VMEM((2, 2, ROWS * half_len, HEAD_DIM), f32),
            pltpu.VMEM((2, ROWS, tok_rows, TILE), bf16),
            pltpu.VMEM((toks, TILE), bf16),
            pltpu.VMEM((2, ROWS, fold, 2, GROUP, half_len, HEAD_DIM), bf16),
            pltpu.VMEM((2, toks, inner), bf16),
            pltpu.VMEM((2, ROWS, tok_rows, TILE), bf16),
            pltpu.VMEM((2, STEP_HEADS, 2, group_cols // HEAD_DIM, half_len, HEAD_DIM), bf16),
            pltpu.SemaphoreType.DMA((2,)),
            pltpu.SemaphoreType.DMA((2,)),
            pltpu.SemaphoreType.DMA((2,)),
            pltpu.SemaphoreType.DMA((2,)),
            pltpu.SemaphoreType.DMA((2,)),
            pltpu.SemaphoreType.DMA((2,)),
            pltpu.SemaphoreType.DMA((2,)),
            pltpu.SemaphoreType.DMA((2,)),
            pltpu.SemaphoreType.DMA((3,)),
            pltpu.SemaphoreType.DMA((8, 2 * rows)),
            pltpu.SemaphoreType.DMA((8, 2 * rows)),
        ] + attn_scratch(cp, half_len),
        compiler_params=pltpu.CompilerParams(dimension_semantics=('arbitrary',), collective_id=0, has_side_effects=True, vmem_limit_bytes=VMEM_LIMIT),
        cost_estimate=pl.CostEstimate(flops=flops, bytes_accessed=4 * rows * tok_rows * depth, transcendentals=0),
    )(x_loc, cosine, sine, w_query, w_key, w_value, w_out)
    return y


def solution(mesh):
    row_spec, pos_spec, rep_spec = P('data', 'cp', None), P('data', 'cp'), P(None, None)

    def local_block(x_loc, pos_loc, w_query, w_key, w_value, w_out):
        cosine, sine = rope_tables(pos_loc)
        return layer(mesh, x_loc, cosine, sine, w_query, w_key, w_value, w_out)

    return jax.shard_map(local_block, mesh=mesh, in_specs=(row_spec, pos_spec, rep_spec, rep_spec, rep_spec, rep_spec), out_specs=row_spec, check_vma=False)
```
